256 devices in a mesh: gz: 256 (over z, y, x, core).
Axes of the slice: x: 4, y: 4, z: 8, core: 2. Of those that a mesh axis runs over, the one named last changes fastest.
Arguments:
- coefficient: float32 [512, 512, 512], P('gz'), may hold values from 0.2 to 1.3
- initial_field: float32 [512, 512, 512], P('gz'), may hold values from -6 to 6
- observed: float32 [512, 512, 512], P('gz'), may hold values from -6 to 6
- misfit_weight: float32 [512, 512, 512], P('gz'), may hold values from 0.5 to 6, as said below
Outputs:
- coeff_gradient: float32 [512, 512, 512], P('gz')
- adjoint_field: float32 [512, 512, 512], P('gz')
- misfit: float32 [], replicated
The draws below stay inside these ranges and needn't reach their ends.
Inputs may be any that keep to these rules, and one draw needn't show every extreme that they name: `misfit_weight`: positive cell weights.
All inputs are finite; a program needn't handle non-finite values.
Results may differ from the reference program's by a relative error of at most 0.00002.
Values sent between devices are 32-bit elements; how exact they have to be, the bound alone decides.
A program may use at most 128 MiB of HBM per device.

```python
import math
import jax
import jax.numpy as jnp

NY = 512
NX = 512
ITERS = 4
NZ = 512


def draw_misfit_weight(key, part):
    depth = jnp.arange(NZ, dtype=jnp.float32)[:, None, None]
    ramp = 1.0 + 2.0 * depth / (NZ - 1)
    base = jnp.exp(jax.random.uniform(key, (NZ, NY, NX), jnp.float32, jnp.log(0.5), jnp.log(2.0)))
    return (ramp * base).astype(jnp.float32)


def block_scale(stream_key, shape, split, smallest, high):
    def one(axis_at, parts):
        steps = jax.random.uniform(jax.random.fold_in(jax.random.fold_in(stream_key, 6), axis_at), (parts,), jnp.float32, smallest / len(split), high / len(split))
        return jnp.repeat(jnp.exp(steps), shape[axis_at] // parts).reshape((-1,) + (1,) * (len(shape) - axis_at - 1))

    gain = one(*split[0])
    for cut in split[1:]:
        gain = gain * one(*cut)
    return gain


def centred(key, extent, width, bound, split=(), kind=jnp.bfloat16):
    array = width * jax.random.normal(key, extent, jnp.float32)
    if split:
        array = array * block_scale(key, extent, split, -0.22, 0.18)
    return jnp.clip(array, -bound, bound).astype(kind)


def setup_inputs(seed: int = 0) -> dict:
    splits = jax.random.split(jax.random.key(seed), 5)
    coefficient = jnp.clip(jnp.exp(math.log(1.3) - 1.8718021 * jax.random.uniform(splits[0], (NZ, NY, NX), jnp.float32) ** block_scale(splits[0], (NZ, NY, NX), ((0, 256),), -0.2, 0.2)), 0.2, 1.3)
    initial_field = centred(splits[1], (NZ, NY, NX), 1.0, 6.0, ((0, 256),), jnp.float32)
    observed = centred(splits[2], (NZ, NY, NX), 1.0, 6.0, ((0, 256),), jnp.float32)
    misfit_weight = draw_misfit_weight(jax.random.fold_in(splits[4], 71), 0)
    return {"coefficient": coefficient, "initial_field": initial_field, "observed": observed, "misfit_weight": misfit_weight}


time_step = 0.125

def laplace(field):
    padded = jnp.pad(field, 1)
    beside = padded[2:, 1:-1, 1:-1] + padded[:-2, 1:-1, 1:-1]
    beside = beside + padded[1:-1, 2:, 1:-1] + padded[1:-1, :-2, 1:-1]
    beside = beside + padded[1:-1, 1:-1, 2:] + padded[1:-1, 1:-1, :-2]
    return beside - 6.0 * field

def reference(coefficient, initial_field, observed, misfit_weight):
    state = initial_field
    slopes = []
    for step in range(ITERS):
        slope = laplace(state)
        slopes.append(slope)
        state = state + time_step * coefficient * slope
    resid = state - observed
    total = jnp.sum(misfit_weight * resid * resid)
    misfit = jnp.sqrt(total / (NZ * NY * NX) + 1e-06)
    adjoint = misfit_weight * resid / misfit
    gradient = jnp.zeros_like(coefficient)
    for step in reversed(range(ITERS)):
        gradient = gradient + time_step * adjoint * slopes[step]
        adjoint = adjoint + time_step * laplace(coefficient * adjoint)
    return (gradient, adjoint, misfit)
```

```python
import functools

import jax
import jax.numpy as jnp
from jax import lax
from jax.experimental import pallas as pl
from jax.experimental.pallas import tpu as pltpu
from jax.sharding import PartitionSpec as P

MESH = pl.DeviceIdType.MESH
time_step = 0.125
ITERS = 4
CHUNKS = 8
PAD = 8
SUB, LANE = 8, 128


def kernel(
    n, ny, nx,
    c_hbm, u_hbm, o_hbm, w_hbm,
    grad_out, lam_out, tot_out,
    u, mu, slopes, c, o, w, lam, grad, ghost, part, incoming,
    load_sem, send_sem, recv_sem, tot_send, tot_recv, out_sem,
):
    me = lax.axis_index("gz")
    core = lax.rem(me, 2)
    beside = me + 1 - 2 * core
    beyond = me - 1 + 2 * core
    inner = jnp.logical_and(me > 0, me < n - 1)
    bits = n.bit_length() - 1
    partners = [me + (1 << b) - 2 * (1 << b) * lax.rem(me // (1 << b), 2) for b in range(bits)]
    rows = ny // CHUNKS
    tiles = nx // LANE

    planes = (core, 1 - core)
    loads = []
    for index, (source, target) in enumerate(((u_hbm, u), (c_hbm, c), (o_hbm, o), (w_hbm, w))):
        for slot in range(2):
            place = u.at[0, slot, pl.ds(PAD, ny), :] if target is u else target.at[slot]
            loads.append(pltpu.make_async_copy(source.at[planes[slot]], place, load_sem.at[index, slot]))
    for load in loads[:4]:
        load.start()

    barrier = pltpu.get_barrier_semaphore()
    for partner in partners:
        pl.semaphore_signal(barrier, inc=1, device_id=(partner,), device_id_type=MESH)

    @pl.when(inner)
    def _():
        pl.semaphore_signal(barrier, inc=1, device_id=(beyond,), device_id_type=MESH)

    pl.semaphore_wait(barrier, bits + inner.astype(jnp.int32))

    def copy_out(source, step, slot, start, count, target):
        return pltpu.make_async_remote_copy(
            src_ref=source,
            dst_ref=ghost.at[step, slot, pl.ds(start, count), :],
            send_sem=send_sem.at[step, slot],
            recv_sem=recv_sem.at[step, slot, start // rows],
            device_id=(target,),
            device_id_type=MESH,
        )

    def send(view, step, start):
        @pl.when(inner)
        def _():
            copy_out(view(0), step, 0, start, rows, beyond).start()

        copy_out(view(1), step, 1, start, rows, beside).start()

    def arrived(step, start):
        @pl.when(inner)
        def _():
            copy_out(ghost.at[step, 0, pl.ds(start, rows), :], step, 0, start, rows, beyond).wait_recv()

        copy_out(ghost.at[step, 1, pl.ds(start, rows), :], step, 1, start, rows, beside).wait_recv()

    for chunk in range(CHUNKS):
        start = chunk * rows
        send(lambda slot: u_hbm.at[planes[slot], pl.ds(start, rows), :], 0, start)
    for load in loads[4:]:
        load.start()

    edge = jnp.zeros((SUB, nx), jnp.float32)
    for field, count in ((u, ITERS), (mu, ITERS)):
        for step in range(count):
            for slot in range(2):
                field[step, slot, pl.ds(PAD - SUB, SUB), :] = edge
                field[step, slot, pl.ds(PAD + ny, SUB), :] = edge

    @pl.when(jnp.logical_not(inner))
    def _():
        def blank(at, carry):
            step, row = at // (ny // SUB), lax.rem(at, ny // SUB)
            ghost[step, 0, pl.ds(pl.multiple_of(row * SUB, SUB), SUB), :] = edge
            return carry

        lax.fori_loop(0, 2 * ITERS * (ny // SUB), blank, 0)

    sublane = lax.broadcasted_iota(jnp.int32, (SUB, LANE), 0)
    lane = lax.broadcasted_iota(jnp.int32, (SUB, LANE), 1)
    top, bottom = sublane == 0, sublane == SUB - 1
    first, last = lane == 0, lane == LANE - 1
    nothing = jnp.zeros((SUB, LANE), jnp.float32)

    def columns(tile):
        return pl.ds(tile * LANE, LANE)

    def laplace(field, step, halo, start, use):
        for slot in range(2):
            def row_of(at):
                at = pl.multiple_of(start + at + PAD, SUB)
                return [field[step, slot, pl.ds(at, SUB), columns(t)] for t in range(tiles)]

            above = [pltpu.roll(x, 1, 0) for x in row_of(-SUB)]
            here = row_of(0)
            here_down = [pltpu.roll(x, SUB - 1, 0) for x in here]
            for at in range(0, rows, SUB):
                below = row_of(at + SUB)
                below_down = [pltpu.roll(x, SUB - 1, 0) for x in below]
                here_up = [pltpu.roll(x, 1, 0) for x in here]
                right = [pltpu.roll(x, 1, 1) for x in here]
                left = [pltpu.roll(x, LANE - 1, 1) for x in here]
                row = pl.multiple_of(start + at, SUB)
                for t in range(tiles):
                    value = here[t]
                    beside_y = jnp.where(top, above[t], here_up[t]) + jnp.where(bottom, below_down[t], here_down[t])
                    before = jnp.where(first, right[t - 1] if t else nothing, right[t])
                    after = jnp.where(last, left[t + 1] if t < tiles - 1 else nothing, left[t])
                    other = field[step, 1 - slot, pl.ds(pl.multiple_of(row + PAD, SUB), SUB), columns(t)]
                    across = other + ghost[halo, slot, pl.ds(row, SUB), columns(t)]
                    lap = (across + beside_y + (before + after)) - 6.0 * value
                    use(slot, row, columns(t), value, lap)
                above, here, here_down = here_up, below, below_down

    for load in loads[:4]:
        load.wait()

    def forward(at, carry):
        step, chunk = at // CHUNKS, lax.rem(at, CHUNKS)
        start = pl.multiple_of(chunk * rows, rows)
        arrived(step, start)

        def use(slot, row, cols, value, lap):
            scaled = time_step * lap
            slopes[step, slot, pl.ds(row, SUB), cols] = scaled
            u[step + 1, slot, pl.ds(pl.multiple_of(row + PAD, SUB), SUB), cols] = (
                value + c[slot, pl.ds(row, SUB), cols] * scaled
            )

        laplace(u, step, step, start, use)
        send(lambda slot: u.at[step + 1, slot, pl.ds(start + PAD, rows), :], step + 1, start)
        return carry

    lax.fori_loop(0, (ITERS - 1) * CHUNKS, forward, 0)
    for load in loads[4:]:
        load.wait()
    part[0] = nothing

    def turn(chunk, carry):
        start = pl.multiple_of(chunk * rows, rows)
        arrived(ITERS - 1, start)
        sums = [nothing, nothing]

        def use(slot, row, cols, value, lap):
            scaled = time_step * lap
            at = (slot, pl.ds(row, SUB), cols)
            coefficient = c[at]
            resid = value + coefficient * scaled - o[at]
            adjoint = w[at] * resid
            sums[slot] = sums[slot] + adjoint * resid
            lam[at] = adjoint
            grad[at] = adjoint * scaled
            mu[0, slot, pl.ds(pl.multiple_of(row + PAD, SUB), SUB), cols] = coefficient * adjoint

        laplace(u, ITERS - 1, ITERS - 1, start, use)
        send(lambda slot: mu.at[0, slot, pl.ds(start + PAD, rows), :], ITERS, start)
        part[0] = part[0] + (sums[0] + sums[1])
        return carry

    lax.fori_loop(0, CHUNKS, turn, 0)

    def total_copy(bit):
        return pltpu.make_async_remote_copy(
            src_ref=part.at[bit],
            dst_ref=incoming.at[bit],
            send_sem=tot_send.at[bit],
            recv_sem=tot_recv.at[bit],
            device_id=(partners[bit],),
            device_id_type=MESH,
        )

    spacing = ITERS * CHUNKS // bits

    def total_step(bit):
        total_copy(bit).wait()
        part[bit + 1] = part[bit] + incoming[bit]

    def total_stages(at, low, high):
        for bit in range(bits):
            if low <= spacing * bit < high:
                @pl.when(at == spacing * bit)
                def _():
                    total_copy(bit).start()

            if low <= spacing * bit + spacing - 1 < high:
                @pl.when(at == spacing * bit + spacing - 1)
                def _():
                    total_step(bit)

    def adjoint(at, carry):
        step, chunk = at // CHUNKS, lax.rem(at, CHUNKS)
        start = pl.multiple_of(chunk * rows, rows)
        total_stages(at, 0, (ITERS - 1) * CHUNKS)
        arrived(ITERS + step, start)

        def use(slot, row, cols, value, lap):
            at = (slot, pl.ds(row, SUB), cols)
            fresh = lam[at] + time_step * lap
            lam[at] = fresh
            grad[at] = grad[at] + fresh * slopes[ITERS - 2 - step, slot, pl.ds(row, SUB), cols]
            mu[step + 1, slot, pl.ds(pl.multiple_of(row + PAD, SUB), SUB), cols] = c[at] * fresh

        laplace(mu, step, ITERS + step, start, use)
        send(lambda slot: mu.at[step + 1, slot, pl.ds(start + PAD, rows), :], ITERS + step + 1, start)
        return carry

    lax.fori_loop(0, (ITERS - 1) * CHUNKS, adjoint, 0)

    outs = [pltpu.make_async_copy(grad.at[slot], grad_out.at[planes[slot]], out_sem.at[0, slot]) for slot in range(2)]
    for out in outs:
        out.start()

    def lam_copy(slot, start, count):
        return pltpu.make_async_copy(
            lam.at[slot, pl.ds(start, count), :],
            lam_out.at[planes[slot], pl.ds(start, count), :],
            out_sem.at[1, slot],
        )

    def finish(chunk, carry):
        start = pl.multiple_of(chunk * rows, rows)
        total_stages(chunk + (ITERS - 1) * CHUNKS, (ITERS - 1) * CHUNKS, ITERS * CHUNKS)
        arrived(2 * ITERS - 1, start)

        def use(slot, row, cols, value, lap):
            at = (slot, pl.ds(row, SUB), cols)
            lam[at] = lam[at] + time_step * lap

        laplace(mu, ITERS - 1, 2 * ITERS - 1, start, use)
        for slot in range(2):
            lam_copy(slot, start, rows).start()
        return carry

    lax.fori_loop(0, CHUNKS, finish, 0)
    total = pltpu.make_async_copy(part.at[bits], tot_out, out_sem.at[2, 0])
    total.start()

    for step in range(2 * ITERS):
        def whole(slot):
            if step == 0:
                return u_hbm.at[planes[slot]]
            return (u.at[step, slot] if step < ITERS else mu.at[step - ITERS, slot]).at[pl.ds(PAD, ny), :]

        @pl.when(inner)
        def _():
            copy_out(whole(0), step, 0, 0, ny, beyond).wait_send()

        copy_out(whole(1), step, 1, 0, ny, beside).wait_send()
    for out in outs:
        out.wait()
    for slot in range(2):
        lam_copy(slot, 0, ny).wait()
    total.wait()


def on_device(n, coefficient, initial_field, observed, misfit_weight):
    depth, ny, nx = coefficient.shape
    bits = n.bit_length() - 1
    anywhere = pl.BlockSpec(memory_space=pl.ANY)
    slab = jax.ShapeDtypeStruct(coefficient.shape, jnp.float32)
    padded = (ITERS, depth, ny + 2 * PAD, nx)
    gradient, adjoint, tile = pl.pallas_call(
        functools.partial(kernel, n, ny, nx),
        out_shape=(slab, slab, jax.ShapeDtypeStruct((SUB, LANE), jnp.float32)),
        in_specs=[anywhere] * 4,
        out_specs=(anywhere,) * 3,
        scratch_shapes=[
            pltpu.VMEM(padded, jnp.float32),
            pltpu.VMEM(padded, jnp.float32),
            pltpu.VMEM((ITERS - 1, depth, ny, nx), jnp.float32),
            pltpu.VMEM((depth, ny, nx), jnp.float32),
            pltpu.VMEM((depth, ny, nx), jnp.float32),
            pltpu.VMEM((depth, ny, nx), jnp.float32),
            pltpu.VMEM((depth, ny, nx), jnp.float32),
            pltpu.VMEM((depth, ny, nx), jnp.float32),
            pltpu.VMEM((2 * ITERS, 2, ny, nx), jnp.float32),
            pltpu.VMEM((bits + 1, SUB, LANE), jnp.float32),
            pltpu.VMEM((bits, SUB, LANE), jnp.float32),
            pltpu.SemaphoreType.DMA((4, 2)),
            pltpu.SemaphoreType.DMA((2 * ITERS, 2)),
            pltpu.SemaphoreType.DMA((2 * ITERS, 2, CHUNKS)),
            pltpu.SemaphoreType.DMA((bits,)),
            pltpu.SemaphoreType.DMA((bits,)),
            pltpu.SemaphoreType.DMA((3, 2)),
        ],
        compiler_params=pltpu.CompilerParams(
            collective_id=0, has_side_effects=True, vmem_limit_bytes=60 * 1024 * 1024
        ),
    )(coefficient, initial_field, observed, misfit_weight)
    cells = n * depth * ny * nx
    misfit = jnp.sqrt(jnp.sum(tile) / cells + 1e-06)
    return gradient / misfit, adjoint / misfit, misfit


def solution(mesh):
    slab = P("gz", None, None)
    return jax.shard_map(
        functools.partial(on_device, mesh.shape["gz"]),
        mesh=mesh,
        in_specs=(slab,) * 4,
        out_specs=(slab, slab, P()),
        check_vma=False,
    )
```

```python
import functools
import itertools
import math

import jax
import jax.numpy as jnp
from jax import lax
from jax.experimental import pallas as pl
from jax.experimental.pallas import tpu as pltpu
from jax.sharding import PartitionSpec as P

MESH = pl.DeviceIdType.MESH
time_step = 0.125
ITERS = 4
CHUNKS = 8
PAD = 8
SUB, LANE = 8, 128
STAGE_TIMES = ((0, 12), (13, 21), (22, None))


def stages(n):
    x = min(4, n // 2)
    y = min(4, n // (2 * x))
    z = n // (2 * x * y)
    return ((2, x),), ((2 * x, y), (1, 2)), ((2 * x * y, z),)


def group_of(me, axes):
    here, base, size = 0, me, math.prod(size for _, size in axes)
    weights = [math.prod(size for _, size in axes[at + 1:]) for at in range(len(axes))]
    places = [lax.rem(me // stride, size) for stride, size in axes]
    for place, weight, (stride, _) in zip(places, weights, axes):
        here, base = here + place * weight, base - place * stride
    others = []
    for turn in itertools.islice(itertools.product(*(range(size) for _, size in axes)), 1, None):
        device, slot = base, 0
        for place, step, weight, (stride, count) in zip(places, turn, weights, axes):
            other = lax.rem(place + step, count)
            device, slot = device + other * stride, slot + other * weight
        others.append((device, slot))
    return here, others


def kernel(
    n, ny, nx,
    c_hbm, u_hbm, o_hbm, w_hbm,
    grad_out, lam_out, tot_out,
    u, mu, slopes, c, o, w, lam, grad, ghost, tiles_of, total_of,
    load_sem, send_sem, recv_sem, tot_send, tot_recv, out_sem,
):
    me = lax.axis_index("gz")
    core = lax.rem(me, 2)
    beside = me + 1 - 2 * core
    beyond = me - 1 + 2 * core
    inner = jnp.logical_and(me > 0, me < n - 1)
    groups = [group_of(me, axes) for axes in stages(n)]
    partners = [device for _, others in groups for device, _ in others]
    rows = ny // CHUNKS
    tiles = nx // LANE

    planes = (core, 1 - core)
    loads = []
    for index, (source, target) in enumerate(((u_hbm, u), (c_hbm, c), (o_hbm, o), (w_hbm, w))):
        for slot in range(2):
            place = u.at[0, slot, pl.ds(PAD, ny), :] if target is u else target.at[slot]
            loads.append(pltpu.make_async_copy(source.at[planes[slot]], place, load_sem.at[index, slot]))
    for load in loads[:4]:
        load.start()

    barrier = pltpu.get_barrier_semaphore()
    for partner in partners:
        pl.semaphore_signal(barrier, inc=1, device_id=(partner,), device_id_type=MESH)

    @pl.when(inner)
    def _():
        pl.semaphore_signal(barrier, inc=1, device_id=(beyond,), device_id_type=MESH)

    pl.semaphore_wait(barrier, len(partners) + inner.astype(jnp.int32))

    def copy_out(source, step, slot, start, count, target):
        return pltpu.make_async_remote_copy(
            src_ref=source,
            dst_ref=ghost.at[step, slot, pl.ds(start, count), :],
            send_sem=send_sem.at[step, slot],
            recv_sem=recv_sem.at[step, slot, start // rows],
            device_id=(target,),
            device_id_type=MESH,
        )

    def send(view, step, start):
        @pl.when(inner)
        def _():
            copy_out(view(0), step, 0, start, rows, beyond).start()

        copy_out(view(1), step, 1, start, rows, beside).start()

    def arrived(step, start):
        @pl.when(inner)
        def _():
            copy_out(ghost.at[step, 0, pl.ds(start, rows), :], step, 0, start, rows, beyond).wait_recv()

        copy_out(ghost.at[step, 1, pl.ds(start, rows), :], step, 1, start, rows, beside).wait_recv()

    for chunk in range(CHUNKS):
        start = chunk * rows
        send(lambda slot: u_hbm.at[planes[slot], pl.ds(start, rows), :], 0, start)
    for load in loads[4:]:
        load.start()

    edge = jnp.zeros((SUB, nx), jnp.float32)
    for field, count in ((u, ITERS), (mu, ITERS)):
        for step in range(count):
            for slot in range(2):
                field[step, slot, pl.ds(PAD - SUB, SUB), :] = edge
                field[step, slot, pl.ds(PAD + ny, SUB), :] = edge

    @pl.when(jnp.logical_not(inner))
    def _():
        def blank(at, carry):
            step, row = at // (ny // SUB), lax.rem(at, ny // SUB)
            ghost[step, 0, pl.ds(pl.multiple_of(row * SUB, SUB), SUB), :] = edge
            return carry

        lax.fori_loop(0, 2 * ITERS * (ny // SUB), blank, 0)

    sublane = lax.broadcasted_iota(jnp.int32, (SUB, LANE), 0)
    lane = lax.broadcasted_iota(jnp.int32, (SUB, LANE), 1)
    top, bottom = sublane == 0, sublane == SUB - 1
    first, last = lane == 0, lane == LANE - 1
    nothing = jnp.zeros((SUB, LANE), jnp.float32)

    def columns(tile):
        return pl.ds(tile * LANE, LANE)

    def laplace(field, step, halo, start, use):
        for slot in range(2):
            def row_of(at):
                at = pl.multiple_of(start + at + PAD, SUB)
                return [field[step, slot, pl.ds(at, SUB), columns(t)] for t in range(tiles)]

            above = [pltpu.roll(x, 1, 0) for x in row_of(-SUB)]
            here = row_of(0)
            here_down = [pltpu.roll(x, SUB - 1, 0) for x in here]
            for at in range(0, rows, SUB):
                below = row_of(at + SUB)
                below_down = [pltpu.roll(x, SUB - 1, 0) for x in below]
                here_up = [pltpu.roll(x, 1, 0) for x in here]
                right = [pltpu.roll(x, 1, 1) for x in here]
                left = [pltpu.roll(x, LANE - 1, 1) for x in here]
                row = pl.multiple_of(start + at, SUB)
                for t in range(tiles):
                    value = here[t]
                    beside_y = jnp.where(top, above[t], here_up[t]) + jnp.where(bottom, below_down[t], here_down[t])
                    before = jnp.where(first, right[t - 1] if t else nothing, right[t])
                    after = jnp.where(last, left[t + 1] if t < tiles - 1 else nothing, left[t])
                    other = field[step, 1 - slot, pl.ds(pl.multiple_of(row + PAD, SUB), SUB), columns(t)]
                    across = other + ghost[halo, slot, pl.ds(row, SUB), columns(t)]
                    lap = (across + beside_y + (before + after)) - 6.0 * value
                    use(slot, row, columns(t), value, lap)
                above, here, here_down = here_up, below, below_down

    for load in loads[:4]:
        load.wait()

    def forward(at, carry):
        step, chunk = at // CHUNKS, lax.rem(at, CHUNKS)
        start = pl.multiple_of(chunk * rows, rows)
        arrived(step, start)

        def use(slot, row, cols, value, lap):
            scaled = time_step * lap
            slopes[step, slot, pl.ds(row, SUB), cols] = scaled
            u[step + 1, slot, pl.ds(pl.multiple_of(row + PAD, SUB), SUB), cols] = (
                value + c[slot, pl.ds(row, SUB), cols] * scaled
            )

        laplace(u, step, step, start, use)
        send(lambda slot: u.at[step + 1, slot, pl.ds(start + PAD, rows), :], step + 1, start)
        return carry

    lax.fori_loop(0, (ITERS - 1) * CHUNKS, forward, 0)
    for load in loads[4:]:
        load.wait()
    total_of[...] = nothing

    def turn(chunk, carry):
        start = pl.multiple_of(chunk * rows, rows)
        arrived(ITERS - 1, start)
        sums = [nothing, nothing]

        def use(slot, row, cols, value, lap):
            scaled = time_step * lap
            at = (slot, pl.ds(row, SUB), cols)
            coefficient = c[at]
            resid = value + coefficient * scaled - o[at]
            adjoint = w[at] * resid
            sums[slot] = sums[slot] + adjoint * resid
            lam[at] = adjoint
            grad[at] = adjoint * scaled
            mu[0, slot, pl.ds(pl.multiple_of(row + PAD, SUB), SUB), cols] = coefficient * adjoint

        laplace(u, ITERS - 1, ITERS - 1, start, use)
        send(lambda slot: mu.at[0, slot, pl.ds(start + PAD, rows), :], ITERS, start)
        total_of[...] = total_of[...] + (sums[0] + sums[1])
        return carry

    lax.fori_loop(0, CHUNKS, turn, 0)

    def tile_copy(stage, device, slot):
        here, _ = groups[stage]
        return pltpu.make_async_remote_copy(
            src_ref=tiles_of.at[stage, here],
            dst_ref=tiles_of.at[stage, here],
            send_sem=tot_send.at[stage, slot],
            recv_sem=tot_recv.at[stage, here],
            device_id=(device,),
            device_id_type=MESH,
        )

    def place(stage):
        tiles_of[stage, groups[stage][0]] = total_of[...]

    def exchange(stage):
        for device, slot in groups[stage][1]:
            tile_copy(stage, device, slot).start()

    def collect(stage):
        for device, slot in groups[stage][1]:
            tile_copy(stage, device, slot).wait_send()
            pltpu.make_async_remote_copy(
                src_ref=tiles_of.at[stage, slot],
                dst_ref=tiles_of.at[stage, slot],
                send_sem=tot_send.at[stage, slot],
                recv_sem=tot_recv.at[stage, slot],
                device_id=(device,),
                device_id_type=MESH,
            ).wait_recv()
        total = tiles_of[stage, 0]
        for slot in range(1, len(groups[stage][1]) + 1):
            total = total + tiles_of[stage, slot]
        total_of[...] = total

    place(0)

    def total_stages(at):
        for stage, (first_at, last_at) in enumerate(STAGE_TIMES):
            @pl.when(at == first_at)
            def _():
                exchange(stage)

            if stage < len(STAGE_TIMES) - 1:
                @pl.when(at == last_at)
                def _():
                    collect(stage)
                    place(stage + 1)

    def adjoint(at, carry):
        step, chunk = at // CHUNKS, lax.rem(at, CHUNKS)
        start = pl.multiple_of(chunk * rows, rows)
        total_stages(at)
        arrived(ITERS + step, start)

        def use(slot, row, cols, value, lap):
            at = (slot, pl.ds(row, SUB), cols)
            fresh = lam[at] + time_step * lap
            lam[at] = fresh
            grad[at] = grad[at] + fresh * slopes[ITERS - 2 - step, slot, pl.ds(row, SUB), cols]
            mu[step + 1, slot, pl.ds(pl.multiple_of(row + PAD, SUB), SUB), cols] = c[at] * fresh

        laplace(mu, step, ITERS + step, start, use)
        send(lambda slot: mu.at[step + 1, slot, pl.ds(start + PAD, rows), :], ITERS + step + 1, start)
        return carry

    lax.fori_loop(0, (ITERS - 1) * CHUNKS, adjoint, 0)

    outs = [pltpu.make_async_copy(grad.at[slot], grad_out.at[planes[slot]], out_sem.at[0, slot]) for slot in range(2)]
    for out in outs:
        out.start()

    def lam_copy(slot, start, count):
        return pltpu.make_async_copy(
            lam.at[slot, pl.ds(start, count), :],
            lam_out.at[planes[slot], pl.ds(start, count), :],
            out_sem.at[1, slot],
        )

    def finish(chunk, carry):
        start = pl.multiple_of(chunk * rows, rows)
        arrived(2 * ITERS - 1, start)

        def use(slot, row, cols, value, lap):
            at = (slot, pl.ds(row, SUB), cols)
            lam[at] = lam[at] + time_step * lap

        laplace(mu, ITERS - 1, 2 * ITERS - 1, start, use)
        for slot in range(2):
            lam_copy(slot, start, rows).start()
        return carry

    lax.fori_loop(0, CHUNKS, finish, 0)
    collect(len(groups) - 1)
    total = pltpu.make_async_copy(total_of, tot_out, out_sem.at[2, 0])
    total.start()

    for step in range(2 * ITERS):
        def whole(slot):
            if step == 0:
                return u_hbm.at[planes[slot]]
            return (u.at[step, slot] if step < ITERS else mu.at[step - ITERS, slot]).at[pl.ds(PAD, ny), :]

        @pl.when(inner)
        def _():
            copy_out(whole(0), step, 0, 0, ny, beyond).wait_send()

        copy_out(whole(1), step, 1, 0, ny, beside).wait_send()
    for out in outs:
        out.wait()
    for slot in range(2):
        lam_copy(slot, 0, ny).wait()
    total.wait()


def on_device(n, coefficient, initial_field, observed, misfit_weight):
    depth, ny, nx = coefficient.shape
    groups = stages(n)
    most = max(math.prod(size for _, size in axes) for axes in groups)
    anywhere = pl.BlockSpec(memory_space=pl.ANY)
    slab = jax.ShapeDtypeStruct(coefficient.shape, jnp.float32)
    padded = (ITERS, depth, ny + 2 * PAD, nx)
    gradient, adjoint, tile = pl.pallas_call(
        functools.partial(kernel, n, ny, nx),
        out_shape=(slab, slab, jax.ShapeDtypeStruct((SUB, LANE), jnp.float32)),
        in_specs=[anywhere] * 4,
        out_specs=(anywhere,) * 3,
        scratch_shapes=[
            pltpu.VMEM(padded, jnp.float32),
            pltpu.VMEM(padded, jnp.float32),
            pltpu.VMEM((ITERS - 1, depth, ny, nx), jnp.float32),
            pltpu.VMEM((depth, ny, nx), jnp.float32),
            pltpu.VMEM((depth, ny, nx), jnp.float32),
            pltpu.VMEM((depth, ny, nx), jnp.float32),
            pltpu.VMEM((depth, ny, nx), jnp.float32),
            pltpu.VMEM((depth, ny, nx), jnp.float32),
            pltpu.VMEM((2 * ITERS, 2, ny, nx), jnp.float32),
            pltpu.VMEM((len(groups), most, SUB, LANE), jnp.float32),
            pltpu.VMEM((SUB, LANE), jnp.float32),
            pltpu.SemaphoreType.DMA((4, 2)),
            pltpu.SemaphoreType.DMA((2 * ITERS, 2)),
            pltpu.SemaphoreType.DMA((2 * ITERS, 2, CHUNKS)),
            pltpu.SemaphoreType.DMA((len(groups), most)),
            pltpu.SemaphoreType.DMA((len(groups), most)),
            pltpu.SemaphoreType.DMA((3, 2)),
        ],
        compiler_params=pltpu.CompilerParams(
            collective_id=0, has_side_effects=True, vmem_limit_bytes=60 * 1024 * 1024
        ),
    )(coefficient, initial_field, observed, misfit_weight)
    cells = n * depth * ny * nx
    misfit = jnp.sqrt(jnp.sum(tile) / cells + 1e-06)
    return gradient / misfit, adjoint / misfit, misfit


def solution(mesh):
    slab = P("gz", None, None)
    return jax.shard_map(
        functools.partial(on_device, mesh.shape["gz"]),
        mesh=mesh,
        in_specs=(slab,) * 4,
        out_specs=(slab, slab, P()),
        check_vma=False,
    )
```

```python
import functools

import jax
import jax.numpy as jnp
from jax import lax
from jax.experimental import pallas as pl
from jax.experimental.pallas import tpu as pltpu
from jax.sharding import PartitionSpec as P

MESH = pl.DeviceIdType.MESH
time_step = 0.125
ITERS = 4
CHUNKS = 8
PAD = 8
SUB, LANE = 8, 128
PAIRS = 5
STAGE_TIMES = ((0, 2), (3, 6), (7, 10), (11, 14), (15, 18), (19, None))
HELLO_TIMES = (2, 8, 14, 20)


def torus(n):
    x = min(4, n // 2)
    y = min(4, n // (2 * x))
    return x, y, n // (2 * x * y)


def kernel(
    n, ny, nx,
    c_hbm, u_hbm, o_hbm, w_hbm,
    grad_out, lam_out, tot_out,
    u, mu, slopes, c, o, w, lam, grad, ghost, totals, inbox, layers,
    load_sem, send_sem, recv_sem, tot_send, tot_recv, out_sem, hello,
):
    me = lax.axis_index("gz")
    core = lax.rem(me, 2)
    beside = me + 1 - 2 * core
    beyond = me - 1 + 2 * core
    inner = jnp.logical_and(me > 0, me < n - 1)
    x, y, z = torus(n)
    layer = 2 * x * y
    row, column, depth = lax.rem(me // (2 * x), y), lax.rem(me // 2, x), me // layer
    line = me - 2 * column - core

    def chip_x(step):
        return line + 2 * lax.rem(column + step % x, x)

    def chip_y(step):
        return me + 2 * x * (lax.rem(row + step % y, y) - row)

    x_steps = sorted({1 % x, -1 % x} - {0})
    y_steps = sorted({1 % y, -1 % y} - {0})
    partners = [beside] + [chip_x(step) + c for step in x_steps for c in range(2)] + [chip_y(step) for step in y_steps]
    line_end = jnp.logical_and(inner, jnp.where(core == 0, column == 0, column == x - 1))
    reach = [step for step in (1, 2, 4) if step < z]

    def along_z(step, act):
        for away in (step, -step):
            @pl.when(jnp.logical_and(depth + away >= 0, depth + away < z))
            def _():
                act(me + away * layer)

        return (depth >= step).astype(jnp.int32) + (depth + step < z).astype(jnp.int32)

    rows = ny // CHUNKS
    tiles = nx // LANE

    planes = (core, 1 - core)
    loads = []
    for index, (source, target) in enumerate(((u_hbm, u), (c_hbm, c), (o_hbm, o), (w_hbm, w))):
        for slot in range(2):
            place = u.at[0, slot, pl.ds(PAD, ny), :] if target is u else target.at[slot]
            loads.append(pltpu.make_async_copy(source.at[planes[slot]], place, load_sem.at[index, slot]))
    for load in loads[:4]:
        load.start()

    barrier = pltpu.get_barrier_semaphore()
    for partner in partners:
        pl.semaphore_signal(barrier, inc=1, device_id=(partner,), device_id_type=MESH)

    def ready(device):
        pl.semaphore_signal(barrier, inc=1, device_id=(device,), device_id_type=MESH)

    @pl.when(line_end)
    def _():
        ready(beyond)

    others = along_z(1, ready) if reach else 0
    pl.semaphore_wait(barrier, len(partners) + line_end.astype(jnp.int32) + others)

    def copy_out(source, step, slot, start, count, target):
        return pltpu.make_async_remote_copy(
            src_ref=source,
            dst_ref=ghost.at[step, slot, pl.ds(start, count), :],
            send_sem=send_sem.at[step, slot],
            recv_sem=recv_sem.at[step, slot, start // rows],
            device_id=(target,),
            device_id_type=MESH,
        )

    def send(view, step, start):
        @pl.when(inner)
        def _():
            copy_out(view(0), step, 0, start, rows, beyond).start()

        copy_out(view(1), step, 1, start, rows, beside).start()

    def arrived(step, start):
        @pl.when(inner)
        def _():
            copy_out(ghost.at[step, 0, pl.ds(start, rows), :], step, 0, start, rows, beyond).wait_recv()

        copy_out(ghost.at[step, 1, pl.ds(start, rows), :], step, 1, start, rows, beside).wait_recv()

    for chunk in range(CHUNKS):
        start = chunk * rows
        send(lambda slot: u_hbm.at[planes[slot], pl.ds(start, rows), :], 0, start)
    for load in loads[4:]:
        load.start()

    edge = jnp.zeros((SUB, nx), jnp.float32)
    for field, count in ((u, ITERS), (mu, ITERS)):
        for step in range(count):
            for slot in range(2):
                field[step, slot, pl.ds(PAD - SUB, SUB), :] = edge
                field[step, slot, pl.ds(PAD + ny, SUB), :] = edge

    @pl.when(jnp.logical_not(inner))
    def _():
        def blank(at, carry):
            step, row = at // (ny // SUB), lax.rem(at, ny // SUB)
            ghost[step, 0, pl.ds(pl.multiple_of(row * SUB, SUB), SUB), :] = edge
            return carry

        lax.fori_loop(0, 2 * ITERS * (ny // SUB), blank, 0)

    sublane = lax.broadcasted_iota(jnp.int32, (SUB, LANE), 0)
    lane = lax.broadcasted_iota(jnp.int32, (SUB, LANE), 1)
    top, bottom = sublane == 0, sublane == SUB - 1
    first, last = lane == 0, lane == LANE - 1
    nothing = jnp.zeros((SUB, LANE), jnp.float32)

    def columns(tile):
        return pl.ds(tile * LANE, LANE)

    def laplace(field, step, halo, start, use):
        for slot in range(2):
            def row_of(at):
                at = pl.multiple_of(start + at + PAD, SUB)
                return [field[step, slot, pl.ds(at, SUB), columns(t)] for t in range(tiles)]

            above = [pltpu.roll(x, 1, 0) for x in row_of(-SUB)]
            here = row_of(0)
            here_down = [pltpu.roll(x, SUB - 1, 0) for x in here]
            for at in range(0, rows, SUB):
                below = row_of(at + SUB)
                below_down = [pltpu.roll(x, SUB - 1, 0) for x in below]
                here_up = [pltpu.roll(x, 1, 0) for x in here]
                right = [pltpu.roll(x, 1, 1) for x in here]
                left = [pltpu.roll(x, LANE - 1, 1) for x in here]
                row = pl.multiple_of(start + at, SUB)
                for t in range(tiles):
                    value = here[t]
                    beside_y = jnp.where(top, above[t], here_up[t]) + jnp.where(bottom, below_down[t], here_down[t])
                    before = jnp.where(first, right[t - 1] if t else nothing, right[t])
                    after = jnp.where(last, left[t + 1] if t < tiles - 1 else nothing, left[t])
                    other = field[step, 1 - slot, pl.ds(pl.multiple_of(row + PAD, SUB), SUB), columns(t)]
                    across = other + ghost[halo, slot, pl.ds(row, SUB), columns(t)]
                    lap = (across + beside_y + (before + after)) - 6.0 * value
                    use(slot, row, columns(t), value, lap)
                above, here, here_down = here_up, below, below_down

    for load in loads[:4]:
        load.wait()

    def greet(at):
        for turn in range(len(reach) + 1):
            @pl.when(at == HELLO_TIMES[turn])
            def _():
                if turn > 0:
                    pl.semaphore_wait(hello.at[turn - 1], along_z(reach[turn - 1], lambda device: None))
                if turn < len(reach):
                    along_z(reach[turn], lambda device: pl.semaphore_signal(
                        hello.at[turn], inc=1, device_id=(device,), device_id_type=MESH
                    ))

    def forward(at, carry):
        greet(at)
        step, chunk = at // CHUNKS, lax.rem(at, CHUNKS)
        start = pl.multiple_of(chunk * rows, rows)
        arrived(step, start)

        def use(slot, row, cols, value, lap):
            scaled = time_step * lap
            slopes[step, slot, pl.ds(row, SUB), cols] = scaled
            u[step + 1, slot, pl.ds(pl.multiple_of(row + PAD, SUB), SUB), cols] = (
                value + c[slot, pl.ds(row, SUB), cols] * scaled
            )

        laplace(u, step, step, start, use)
        send(lambda slot: u.at[step + 1, slot, pl.ds(start + PAD, rows), :], step + 1, start)
        return carry

    lax.fori_loop(0, (ITERS - 1) * CHUNKS, forward, 0)
    for load in loads[4:]:
        load.wait()
    totals[0] = nothing

    def turn(chunk, carry):
        start = pl.multiple_of(chunk * rows, rows)
        arrived(ITERS - 1, start)
        sums = [nothing, nothing]

        def use(slot, row, cols, value, lap):
            scaled = time_step * lap
            at = (slot, pl.ds(row, SUB), cols)
            coefficient = c[at]
            resid = value + coefficient * scaled - o[at]
            adjoint = w[at] * resid
            sums[slot] = sums[slot] + adjoint * resid
            lam[at] = adjoint
            grad[at] = adjoint * scaled
            mu[0, slot, pl.ds(pl.multiple_of(row + PAD, SUB), SUB), cols] = coefficient * adjoint

        laplace(u, ITERS - 1, ITERS - 1, start, use)
        send(lambda slot: mu.at[0, slot, pl.ds(start + PAD, rows), :], ITERS, start)
        totals[0] = totals[0] + (sums[0] + sums[1])
        return carry

    lax.fori_loop(0, CHUNKS, turn, 0)

    def tile_copy(source, target, stage, slot, device):
        return pltpu.make_async_remote_copy(
            src_ref=source,
            dst_ref=target,
            send_sem=tot_send.at[stage, slot],
            recv_sem=tot_recv.at[stage, slot],
            device_id=(device,),
            device_id_type=MESH,
        )

    def pair_copy(stage, device, slot=0):
        return tile_copy(totals.at[stage], inbox.at[stage], stage, slot, device)

    def pair_sends(stage, act):
        if stage == 0:
            act(pair_copy(0, beside))
        elif stage < 3:
            upper = lax.rem(column + stage - 1, 2) == 1
            for step, sender in ((1, 0), (-1, 1)):
                @pl.when(jnp.logical_and(core == sender, upper == (step == -1)))
                def _():
                    for c in range(2):
                        act(tile_copy(totals.at[stage], inbox.at[stage], stage, c, chip_x(step) + c))
        else:
            upper = lax.rem(row + stage - 3, 2) == 1
            act(pair_copy(stage, jnp.where(upper, chip_y(-1), chip_y(1))))

    def pair_there(stage):
        return stage == 0 or (x, x // 2, y, y // 2)[stage - 1] > 1

    def layer_copies(act):
        for step in range(1, z):
            device = lax.rem(depth + step, z) * layer + lax.rem(me, layer)
            act(step, device)

    def exchange(stage):
        if stage < PAIRS:
            if pair_there(stage):
                pair_sends(stage, lambda copy: copy.start())
        else:
            def start(step, device):
                tile_copy(layers.at[depth], layers.at[depth], stage, step, device).start()

            layer_copies(start)

    def collect(stage):
        if stage < PAIRS:
            if not pair_there(stage):
                totals[stage + 1] = totals[stage]
                return
            pair_sends(stage, lambda copy: copy.wait_send())
            if 0 < stage < 3:
                for c in range(2):
                    @pl.when(core == c)
                    def _():
                        pair_copy(stage, beside, c).wait_recv()
            else:
                pair_copy(stage, beside).wait_recv()
            totals[stage + 1] = totals[stage] + inbox[stage]
        else:
            def finish(step, device):
                tile_copy(layers.at[depth], layers.at[depth], stage, step, device).wait()

            layer_copies(finish)
            total = layers[0]
            for slot in range(1, z):
                total = total + layers[slot]
            totals[stage + 1] = total

    def total_stages(at):
        for stage, (first_at, last_at) in enumerate(STAGE_TIMES):
            @pl.when(at == first_at)
            def _():
                exchange(stage)

            if stage < PAIRS:
                @pl.when(at == last_at)
                def _():
                    collect(stage)
                    if stage == PAIRS - 1:
                        layers[depth] = totals[PAIRS]

    def adjoint(at, carry):
        step, chunk = at // CHUNKS, lax.rem(at, CHUNKS)
        start = pl.multiple_of(chunk * rows, rows)
        total_stages(at)
        arrived(ITERS + step, start)

        def use(slot, row, cols, value, lap):
            at = (slot, pl.ds(row, SUB), cols)
            fresh = lam[at] + time_step * lap
            lam[at] = fresh
            grad[at] = grad[at] + fresh * slopes[ITERS - 2 - step, slot, pl.ds(row, SUB), cols]
            mu[step + 1, slot, pl.ds(pl.multiple_of(row + PAD, SUB), SUB), cols] = c[at] * fresh

        laplace(mu, step, ITERS + step, start, use)
        send(lambda slot: mu.at[step + 1, slot, pl.ds(start + PAD, rows), :], ITERS + step + 1, start)
        return carry

    lax.fori_loop(0, (ITERS - 1) * CHUNKS, adjoint, 0)

    outs = [pltpu.make_async_copy(grad.at[slot], grad_out.at[planes[slot]], out_sem.at[0, slot]) for slot in range(2)]
    for out in outs:
        out.start()

    def lam_copy(slot, start, count):
        return pltpu.make_async_copy(
            lam.at[slot, pl.ds(start, count), :],
            lam_out.at[planes[slot], pl.ds(start, count), :],
            out_sem.at[1, slot],
        )

    def finish(chunk, carry):
        start = pl.multiple_of(chunk * rows, rows)
        arrived(2 * ITERS - 1, start)

        def use(slot, row, cols, value, lap):
            at = (slot, pl.ds(row, SUB), cols)
            lam[at] = lam[at] + time_step * lap

        laplace(mu, ITERS - 1, 2 * ITERS - 1, start, use)
        for slot in range(2):
            lam_copy(slot, start, rows).start()
        return carry

    lax.fori_loop(0, CHUNKS, finish, 0)
    collect(PAIRS)
    total = pltpu.make_async_copy(totals.at[PAIRS + 1], tot_out, out_sem.at[2, 0])
    total.start()

    for step in range(2 * ITERS):
        def whole(slot):
            if step == 0:
                return u_hbm.at[planes[slot]]
            return (u.at[step, slot] if step < ITERS else mu.at[step - ITERS, slot]).at[pl.ds(PAD, ny), :]

        @pl.when(inner)
        def _():
            copy_out(whole(0), step, 0, 0, ny, beyond).wait_send()

        copy_out(whole(1), step, 1, 0, ny, beside).wait_send()
    for out in outs:
        out.wait()
    for slot in range(2):
        lam_copy(slot, 0, ny).wait()
    total.wait()


def on_device(n, coefficient, initial_field, observed, misfit_weight):
    depth, ny, nx = coefficient.shape
    layers = torus(n)[2]
    anywhere = pl.BlockSpec(memory_space=pl.ANY)
    slab = jax.ShapeDtypeStruct(coefficient.shape, jnp.float32)
    padded = (ITERS, depth, ny + 2 * PAD, nx)
    gradient, adjoint, tile = pl.pallas_call(
        functools.partial(kernel, n, ny, nx),
        out_shape=(slab, slab, jax.ShapeDtypeStruct((SUB, LANE), jnp.float32)),
        in_specs=[anywhere] * 4,
        out_specs=(anywhere,) * 3,
        scratch_shapes=[
            pltpu.VMEM(padded, jnp.float32),
            pltpu.VMEM(padded, jnp.float32),
            pltpu.VMEM((ITERS - 1, depth, ny, nx), jnp.float32),
            pltpu.VMEM((depth, ny, nx), jnp.float32),
            pltpu.VMEM((depth, ny, nx), jnp.float32),
            pltpu.VMEM((depth, ny, nx), jnp.float32),
            pltpu.VMEM((depth, ny, nx), jnp.float32),
            pltpu.VMEM((depth, ny, nx), jnp.float32),
            pltpu.VMEM((2 * ITERS, 2, ny, nx), jnp.float32),
            pltpu.VMEM((PAIRS + 2, SUB, LANE), jnp.float32),
            pltpu.VMEM((PAIRS, SUB, LANE), jnp.float32),
            pltpu.VMEM((layers, SUB, LANE), jnp.float32),
            pltpu.SemaphoreType.DMA((4, 2)),
            pltpu.SemaphoreType.DMA((2 * ITERS, 2)),
            pltpu.SemaphoreType.DMA((2 * ITERS, 2, CHUNKS)),
            pltpu.SemaphoreType.DMA((PAIRS + 1, max(layers, 2))),
            pltpu.SemaphoreType.DMA((PAIRS + 1, max(layers, 2))),
            pltpu.SemaphoreType.DMA((3, 2)),
            pltpu.SemaphoreType.REGULAR((3,)),
        ],
        compiler_params=pltpu.CompilerParams(
            collective_id=0, has_side_effects=True, vmem_limit_bytes=60 * 1024 * 1024
        ),
    )(coefficient, initial_field, observed, misfit_weight)
    cells = n * depth * ny * nx
    misfit = jnp.sqrt(jnp.sum(tile) / cells + 1e-06)
    return gradient / misfit, adjoint / misfit, misfit


def solution(mesh):
    slab = P("gz", None, None)
    return jax.shard_map(
        functools.partial(on_device, mesh.shape["gz"]),
        mesh=mesh,
        in_specs=(slab,) * 4,
        out_specs=(slab, slab, P()),
        check_vma=False,
    )
```

```python
import functools

import jax
import jax.numpy as jnp
from jax import lax
from jax.experimental import pallas as pl
from jax.experimental.pallas import tpu as pltpu
from jax.sharding import PartitionSpec as P

MESH = pl.DeviceIdType.MESH
time_step = 0.125
ITERS = 4
CHUNKS = 8
PAD = 8
SUB, LANE = 8, 128
PIECES = 4
PAIRS = 5
STAGE_TIMES = ((0, 2), (3, 6), (7, 10), (11, 14), (15, 18), (19, None))
HELLO_TIMES = (2, 8, 14, 20)


def torus(n):
    x = min(4, n // 2)
    y = min(4, n // (2 * x))
    return x, y, n // (2 * x * y)


def kernel(
    n, ny, nx,
    c_hbm, u_hbm, o_hbm, w_hbm,
    grad, lam, tot_out,
    u, mu, slopes, c, o, w, ghost, totals, inbox, layers,
    load_sem, send_sem, recv_sem, tot_send, tot_recv, hello,
):
    me = lax.axis_index("gz")
    core = lax.rem(me, 2)
    beside = me + 1 - 2 * core
    beyond = me - 1 + 2 * core
    inner = jnp.logical_and(me > 0, me < n - 1)
    x, y, z = torus(n)
    layer = 2 * x * y
    row, column, depth = lax.rem(me // (2 * x), y), lax.rem(me // 2, x), me // layer
    line = me - 2 * column - core

    def chip_x(step):
        return line + 2 * lax.rem(column + step % x, x)

    def chip_y(step):
        return me + 2 * x * (lax.rem(row + step % y, y) - row)

    x_steps = sorted({1 % x, -1 % x} - {0})
    y_steps = sorted({1 % y, -1 % y} - {0})
    partners = [beside] + [chip_x(step) + c for step in x_steps for c in range(2)] + [chip_y(step) for step in y_steps]
    line_end = jnp.logical_and(inner, jnp.where(core == 0, column == 0, column == x - 1))
    reach = [step for step in (1, 2, 4) if step < z]

    def along_z(step, act):
        for away in (step, -step):
            @pl.when(jnp.logical_and(depth + away >= 0, depth + away < z))
            def _():
                act(me + away * layer)

        return (depth >= step).astype(jnp.int32) + (depth + step < z).astype(jnp.int32)

    rows = ny // CHUNKS
    tiles = nx // LANE

    planes = (core, 1 - core)
    loads = []
    for index, (source, target) in enumerate(((u_hbm, u), (c_hbm, c), (o_hbm, o), (w_hbm, w))):
        for slot in range(2):
            place = u.at[0, slot, pl.ds(PAD, ny), :] if target is u else target.at[slot]
            loads.append(pltpu.make_async_copy(source.at[planes[slot]], place, load_sem.at[index, slot]))
    for load in loads[:4]:
        load.start()

    barrier = pltpu.get_barrier_semaphore()
    for partner in partners:
        pl.semaphore_signal(barrier, inc=1, device_id=(partner,), device_id_type=MESH)

    def ready(device):
        pl.semaphore_signal(barrier, inc=1, device_id=(device,), device_id_type=MESH)

    @pl.when(line_end)
    def _():
        ready(beyond)

    others = along_z(1, ready) if reach else 0
    pl.semaphore_wait(barrier, len(partners) + line_end.astype(jnp.int32) + others)

    def copy_out(source, step, slot, start, count, target):
        return pltpu.make_async_remote_copy(
            src_ref=source,
            dst_ref=ghost.at[step, slot, pl.ds(start, count), :],
            send_sem=send_sem.at[step, slot],
            recv_sem=recv_sem.at[step, slot, start // rows],
            device_id=(target,),
            device_id_type=MESH,
        )

    def send(view, step, start):
        @pl.when(inner)
        def _():
            copy_out(view(0), step, 0, start, rows, beyond).start()

        copy_out(view(1), step, 1, start, rows, beside).start()

    def arrived(step, start):
        @pl.when(inner)
        def _():
            copy_out(ghost.at[step, 0, pl.ds(start, rows), :], step, 0, start, rows, beyond).wait_recv()

        copy_out(ghost.at[step, 1, pl.ds(start, rows), :], step, 1, start, rows, beside).wait_recv()

    for chunk in range(CHUNKS):
        start = chunk * rows
        send(lambda slot: u_hbm.at[planes[slot], pl.ds(start, rows), :], 0, start)
    for load in loads[4:]:
        load.start()

    edge = jnp.zeros((SUB, nx), jnp.float32)
    for field, count in ((u, ITERS), (mu, ITERS)):
        for step in range(count):
            for slot in range(2):
                field[step, slot, pl.ds(PAD - SUB, SUB), :] = edge
                field[step, slot, pl.ds(PAD + ny, SUB), :] = edge

    @pl.when(jnp.logical_not(inner))
    def _():
        def blank(at, carry):
            step, row = at // (ny // SUB), lax.rem(at, ny // SUB)
            ghost[step, 0, pl.ds(pl.multiple_of(row * SUB, SUB), SUB), :] = edge
            return carry

        lax.fori_loop(0, 2 * ITERS * (ny // SUB), blank, 0)

    sublane = lax.broadcasted_iota(jnp.int32, (SUB, LANE), 0)
    lane = lax.broadcasted_iota(jnp.int32, (SUB, LANE), 1)
    top, bottom = sublane == 0, sublane == SUB - 1
    first, last = lane == 0, lane == LANE - 1
    nothing = jnp.zeros((SUB, LANE), jnp.float32)

    def columns(tile):
        return pl.ds(tile * LANE, LANE)

    def laplace(field, step, halo, start, use):
        for slot in range(2):
            def row_of(at):
                at = pl.multiple_of(start + at + PAD, SUB)
                return [field[step, slot, pl.ds(at, SUB), columns(t)] for t in range(tiles)]

            above = [pltpu.roll(x, 1, 0) for x in row_of(-SUB)]
            here = row_of(0)
            here_down = [pltpu.roll(x, SUB - 1, 0) for x in here]
            for at in range(0, rows, SUB):
                below = row_of(at + SUB)
                below_down = [pltpu.roll(x, SUB - 1, 0) for x in below]
                here_up = [pltpu.roll(x, 1, 0) for x in here]
                right = [pltpu.roll(x, 1, 1) for x in here]
                left = [pltpu.roll(x, LANE - 1, 1) for x in here]
                row = pl.multiple_of(start + at, SUB)
                for t in range(tiles):
                    value = here[t]
                    beside_y = jnp.where(top, above[t], here_up[t]) + jnp.where(bottom, below_down[t], here_down[t])
                    before = jnp.where(first, right[t - 1] if t else nothing, right[t])
                    after = jnp.where(last, left[t + 1] if t < tiles - 1 else nothing, left[t])
                    other = field[step, 1 - slot, pl.ds(pl.multiple_of(row + PAD, SUB), SUB), columns(t)]
                    across = other + ghost[halo, slot, pl.ds(row, SUB), columns(t)]
                    lap = (across + beside_y + (before + after)) - 6.0 * value
                    use(slot, row, columns(t), value, lap)
                above, here, here_down = here_up, below, below_down

    for load in loads[:4]:
        load.wait()

    def greet(at):
        for turn in range(len(reach) + 1):
            @pl.when(at == HELLO_TIMES[turn])
            def _():
                if turn > 0:
                    pl.semaphore_wait(hello.at[turn - 1], along_z(reach[turn - 1], lambda device: None))
                if turn < len(reach):
                    along_z(reach[turn], lambda device: pl.semaphore_signal(
                        hello.at[turn], inc=1, device_id=(device,), device_id_type=MESH
                    ))

    def forward(at, carry):
        greet(at)
        step, chunk = at // CHUNKS, lax.rem(at, CHUNKS)
        start = pl.multiple_of(chunk * rows, rows)
        arrived(step, start)

        def use(slot, row, cols, value, lap):
            scaled = time_step * lap
            slopes[step, slot, pl.ds(row, SUB), cols] = scaled
            u[step + 1, slot, pl.ds(pl.multiple_of(row + PAD, SUB), SUB), cols] = (
                value + c[slot, pl.ds(row, SUB), cols] * scaled
            )

        laplace(u, step, step, start, use)
        send(lambda slot: u.at[step + 1, slot, pl.ds(start + PAD, rows), :], step + 1, start)
        return carry

    lax.fori_loop(0, (ITERS - 1) * CHUNKS, forward, 0)
    for load in loads[4:]:
        load.wait()
    totals[0] = nothing

    def turn(chunk, carry):
        start = pl.multiple_of(chunk * rows, rows)
        arrived(ITERS - 1, start)
        sums = [nothing, nothing]

        def use(slot, row, cols, value, lap):
            scaled = time_step * lap
            at = (slot, pl.ds(row, SUB), cols)
            coefficient = c[at]
            resid = value + coefficient * scaled - o[at]
            adjoint = w[at] * resid
            sums[slot] = sums[slot] + adjoint * resid
            lam[at] = adjoint
            grad[at] = adjoint * scaled
            mu[0, slot, pl.ds(pl.multiple_of(row + PAD, SUB), SUB), cols] = coefficient * adjoint

        laplace(u, ITERS - 1, ITERS - 1, start, use)
        send(lambda slot: mu.at[0, slot, pl.ds(start + PAD, rows), :], ITERS, start)
        totals[0] = totals[0] + (sums[0] + sums[1])
        return carry

    lax.fori_loop(0, CHUNKS, turn, 0)

    def tile_copy(source, target, stage, slot, device):
        return pltpu.make_async_remote_copy(
            src_ref=source,
            dst_ref=target,
            send_sem=tot_send.at[stage, slot],
            recv_sem=tot_recv.at[stage, slot],
            device_id=(device,),
            device_id_type=MESH,
        )

    def pair_copy(stage, device, slot=0):
        return tile_copy(totals.at[stage], inbox.at[stage], stage, slot, device)

    def pair_sends(stage, act):
        if stage == 0:
            act(pair_copy(0, beside))
        elif stage < 3:
            upper = lax.rem(column + stage - 1, 2) == 1
            for step, sender in ((1, 0), (-1, 1)):
                @pl.when(jnp.logical_and(core == sender, upper == (step == -1)))
                def _():
                    for c in range(2):
                        act(tile_copy(totals.at[stage], inbox.at[stage], stage, c, chip_x(step) + c))
        else:
            upper = lax.rem(row + stage - 3, 2) == 1
            act(pair_copy(stage, jnp.where(upper, chip_y(-1), chip_y(1))))

    def pair_there(stage):
        return stage == 0 or (x, x // 2, y, y // 2)[stage - 1] > 1

    def layer_copies(act):
        for step in range(1, z):
            device = lax.rem(depth + step, z) * layer + lax.rem(me, layer)
            act(step, device)

    def exchange(stage):
        if stage < PAIRS:
            if pair_there(stage):
                pair_sends(stage, lambda copy: copy.start())
        else:
            def start(step, device):
                tile_copy(layers.at[depth], layers.at[depth], stage, step, device).start()

            layer_copies(start)

    def collect(stage):
        if stage < PAIRS:
            if not pair_there(stage):
                totals[stage + 1] = totals[stage]
                return
            pair_sends(stage, lambda copy: copy.wait_send())
            if 0 < stage < 3:
                for c in range(2):
                    @pl.when(core == c)
                    def _():
                        pair_copy(stage, beside, c).wait_recv()
            else:
                pair_copy(stage, beside).wait_recv()
            totals[stage + 1] = totals[stage] + inbox[stage]
        else:
            def finish(step, device):
                tile_copy(layers.at[depth], layers.at[depth], stage, step, device).wait()

            layer_copies(finish)
            total = layers[0]
            for slot in range(1, z):
                total = total + layers[slot]
            totals[stage + 1] = total

    def total_stages(at):
        for stage, (first_at, last_at) in enumerate(STAGE_TIMES):
            @pl.when(at == first_at)
            def _():
                exchange(stage)

            if stage < PAIRS:
                @pl.when(at == last_at)
                def _():
                    collect(stage)
                    if stage == PAIRS - 1:
                        layers[depth] = totals[PAIRS]

    def adjoint(at, carry):
        step, chunk = at // CHUNKS, lax.rem(at, CHUNKS)
        start = pl.multiple_of(chunk * rows, rows)
        total_stages(at)
        arrived(ITERS + step, start)

        def use(slot, row, cols, value, lap):
            at = (slot, pl.ds(row, SUB), cols)
            fresh = lam[at] + time_step * lap
            lam[at] = fresh
            grad[at] = grad[at] + fresh * slopes[ITERS - 2 - step, slot, pl.ds(row, SUB), cols]
            mu[step + 1, slot, pl.ds(pl.multiple_of(row + PAD, SUB), SUB), cols] = c[at] * fresh

        laplace(mu, step, ITERS + step, start, use)
        send(lambda slot: mu.at[step + 1, slot, pl.ds(start + PAD, rows), :], ITERS + step + 1, start)
        return carry

    lax.fori_loop(0, (ITERS - 1) * CHUNKS, adjoint, 0)

    def finish(chunk, carry):
        start = pl.multiple_of(chunk * rows, rows)
        arrived(2 * ITERS - 1, start)

        def use(slot, row, cols, value, lap):
            at = (slot, pl.ds(row, SUB), cols)
            lam[at] = lam[at] + time_step * lap

        laplace(mu, ITERS - 1, 2 * ITERS - 1, start, use)
        return carry

    lax.fori_loop(0, CHUNKS, finish, 0)
    collect(PAIRS)
    tot_out[...] = totals[PAIRS + 1]

    for step in range(2 * ITERS):
        def whole(slot):
            if step == 0:
                return u_hbm.at[planes[slot]]
            return (u.at[step, slot] if step < ITERS else mu.at[step - ITERS, slot]).at[pl.ds(PAD, ny), :]

        @pl.when(inner)
        def _():
            copy_out(whole(0), step, 0, 0, ny, beyond).wait_send()

        copy_out(whole(1), step, 1, 0, ny, beside).wait_send()


def scale_kernel(cells, grad, lam, tile, grad_out, lam_out, misfit_out, scaled_grad, scaled_lam, out_sem):
    core = lax.rem(lax.axis_index("gz"), 2)
    ny = grad.shape[1]
    rows = ny // PIECES
    misfit = jnp.sqrt(jnp.sum(tile[...], keepdims=True) / cells + 1e-06)
    factor = 1.0 / misfit
    copies = []
    for which, (source, scaled, target) in enumerate(((grad, scaled_grad, grad_out), (lam, scaled_lam, lam_out))):
        for slot in range(2):
            for piece in range(PIECES):
                part = pl.ds(piece * rows, rows)
                scaled[slot, part, :] = source[slot, part, :] * factor
                plane = core if slot == 0 else 1 - core
                copies.append(
                    pltpu.make_async_copy(
                        scaled.at[slot, part, :], target.at[plane, part, :], out_sem.at[which, slot, piece]
                    )
                )
                copies[-1].start()
    misfit_out[0, 0] = misfit[0, 0]
    for copy in copies:
        copy.wait()


def on_device(n, coefficient, initial_field, observed, misfit_weight):
    depth, ny, nx = coefficient.shape
    layers = torus(n)[2]
    far = pl.BlockSpec(memory_space=pltpu.HBM)
    near = pl.BlockSpec(memory_space=pltpu.VMEM)
    slab = jax.ShapeDtypeStruct(coefficient.shape, jnp.float32)
    padded = (ITERS, depth, ny + 2 * PAD, nx)
    gradient, adjoint, tile = pl.pallas_call(
        functools.partial(kernel, n, ny, nx),
        out_shape=(slab, slab, jax.ShapeDtypeStruct((SUB, LANE), jnp.float32)),
        in_specs=[far] * 4,
        out_specs=(near,) * 3,
        scratch_shapes=[
            pltpu.VMEM(padded, jnp.float32),
            pltpu.VMEM(padded, jnp.float32),
            pltpu.VMEM((ITERS - 1, depth, ny, nx), jnp.float32),
            pltpu.VMEM((depth, ny, nx), jnp.float32),
            pltpu.VMEM((depth, ny, nx), jnp.float32),
            pltpu.VMEM((depth, ny, nx), jnp.float32),
            pltpu.VMEM((2 * ITERS, 2, ny, nx), jnp.float32),
            pltpu.VMEM((PAIRS + 2, SUB, LANE), jnp.float32),
            pltpu.VMEM((PAIRS, SUB, LANE), jnp.float32),
            pltpu.VMEM((layers, SUB, LANE), jnp.float32),
            pltpu.SemaphoreType.DMA((4, 2)),
            pltpu.SemaphoreType.DMA((2 * ITERS, 2)),
            pltpu.SemaphoreType.DMA((2 * ITERS, 2, CHUNKS)),
            pltpu.SemaphoreType.DMA((PAIRS + 1, max(layers, 2))),
            pltpu.SemaphoreType.DMA((PAIRS + 1, max(layers, 2))),
            pltpu.SemaphoreType.REGULAR((3,)),
        ],
        compiler_params=pltpu.CompilerParams(
            collective_id=0, has_side_effects=True, vmem_limit_bytes=48 * 1024 * 1024
        ),
    )(coefficient, initial_field, observed, misfit_weight)
    gradient, adjoint, misfit = pl.pallas_call(
        functools.partial(scale_kernel, n * depth * ny * nx),
        out_shape=(slab, slab, jax.ShapeDtypeStruct((1, 1), jnp.float32)),
        in_specs=[near] * 3,
        out_specs=(far, far, pl.BlockSpec(memory_space=pltpu.SMEM)),
        scratch_shapes=[
            pltpu.VMEM((depth, ny, nx), jnp.float32),
            pltpu.VMEM((depth, ny, nx), jnp.float32),
            pltpu.SemaphoreType.DMA((2, 2, PIECES)),
        ],
        compiler_params=pltpu.CompilerParams(vmem_limit_bytes=8 * 1024 * 1024),
    )(gradient, adjoint, tile)
    return gradient, adjoint, misfit.reshape(())


def solution(mesh):
    slab = P("gz", None, None)
    return jax.shard_map(
        functools.partial(on_device, mesh.shape["gz"]),
        mesh=mesh,
        in_specs=(slab,) * 4,
        out_specs=(slab, slab, P()),
        check_vma=False,
    )
```

```python
import functools

import jax
import jax.numpy as jnp
from jax import lax
from jax.experimental import pallas as pl
from jax.experimental.pallas import tpu as pltpu
from jax.sharding import PartitionSpec as P

MESH = pl.DeviceIdType.MESH
time_step = 0.125
ITERS = 4
CHUNKS = 8
PAD = 8
SUB, LANE = 8, 128
SUM_CHUNK = 5
PAIRS = 5
STAGE_TIMES = ((0, 2), (3, 6), (7, 10), (11, 14), (15, 18), (19, None))
HELLO_TIMES = (2, 8, 14, 20)


def torus(n):
    x = min(4, n // 2)
    y = min(4, n // (2 * x))
    return x, y, n // (2 * x * y)


def kernel(
    n, ny, nx,
    c_hbm, u_hbm, o_hbm, w_hbm,
    grad, lam, misfit_out,
    u, mu, slopes, c, o, w, ghost, totals, inbox, layers,
    load_sem, send_sem, recv_sem, tot_send, tot_recv, layer_send, layer_recv, hello,
):
    me = lax.axis_index("gz")
    core = lax.rem(me, 2)
    beside = me + 1 - 2 * core
    beyond = me - 1 + 2 * core
    inner = jnp.logical_and(me > 0, me < n - 1)
    x, y, z = torus(n)
    layer = 2 * x * y
    row, column, depth = lax.rem(me // (2 * x), y), lax.rem(me // 2, x), me // layer
    line = me - 2 * column - core

    def chip_x(step):
        return line + 2 * lax.rem(column + step % x, x)

    def chip_y(step):
        return me + 2 * x * (lax.rem(row + step % y, y) - row)

    x_steps = sorted({1 % x, -1 % x} - {0})
    y_steps = sorted({1 % y, -1 % y} - {0})
    partners = [beside] + [chip_x(step) + c for step in x_steps for c in range(2)] + [chip_y(step) for step in y_steps]
    line_end = jnp.logical_and(inner, jnp.where(core == 0, column == 0, column == x - 1))
    reach = [step for step in (1, 2, 4) if step < z]

    def along_z(step, act):
        for away in (step, -step):
            @pl.when(jnp.logical_and(depth + away >= 0, depth + away < z))
            def _():
                act(me + away * layer)

        return (depth >= step).astype(jnp.int32) + (depth + step < z).astype(jnp.int32)

    rows = ny // CHUNKS
    tiles = nx // LANE

    planes = (core, 1 - core)
    loads = []
    for index, (source, target) in enumerate(((u_hbm, u), (c_hbm, c), (o_hbm, o), (w_hbm, w))):
        for slot in range(2):
            place = u.at[0, slot, pl.ds(PAD, ny), :] if target is u else target.at[slot]
            loads.append(pltpu.make_async_copy(source.at[planes[slot]], place, load_sem.at[index, slot]))
    barrier = pltpu.get_barrier_semaphore()

    def ready(device):
        pl.semaphore_signal(barrier, inc=1, device_id=(device,), device_id_type=MESH)

    @pl.when(line_end)
    def _():
        ready(beyond)

    for partner in partners:
        ready(partner)
    others = along_z(1, ready) if reach else 0
    for load in loads[:4]:
        load.start()
    for load in loads[:2]:
        load.wait()
    pl.semaphore_wait(barrier, len(partners) + line_end.astype(jnp.int32) + others)

    def copy_out(source, step, slot, start, count, target):
        return pltpu.make_async_remote_copy(
            src_ref=source,
            dst_ref=ghost.at[step, slot, pl.ds(start, count), :],
            send_sem=send_sem.at[step, slot],
            recv_sem=recv_sem.at[step % 2 if isinstance(step, int) else lax.rem(step, 2), slot, start // rows],
            device_id=(target,),
            device_id_type=MESH,
        )

    def send(view, step, start):
        @pl.when(inner)
        def _():
            copy_out(view(0), step, 0, start, rows, beyond).start()

        copy_out(view(1), step, 1, start, rows, beside).start()

    def arrived(step, start):
        @pl.when(inner)
        def _():
            copy_out(ghost.at[step, 0, pl.ds(start, rows), :], step, 0, start, rows, beyond).wait_recv()

        copy_out(ghost.at[step, 1, pl.ds(start, rows), :], step, 1, start, rows, beside).wait_recv()

    for chunk in range(CHUNKS):
        start = chunk * rows
        send(lambda slot: u.at[0, slot, pl.ds(PAD + start, rows), :], 0, start)
    for load in loads[4:]:
        load.start()

    edge = jnp.zeros((SUB, nx), jnp.float32)
    for field, count in ((u, ITERS), (mu, ITERS)):
        for step in range(count):
            for slot in range(2):
                field[step, slot, pl.ds(PAD - SUB, SUB), :] = edge
                field[step, slot, pl.ds(PAD + ny, SUB), :] = edge

    @pl.when(jnp.logical_not(inner))
    def _():
        def blank(at, carry):
            step, row = at // (ny // SUB), lax.rem(at, ny // SUB)
            ghost[step, 0, pl.ds(pl.multiple_of(row * SUB, SUB), SUB), :] = edge
            return carry

        lax.fori_loop(0, 2 * ITERS * (ny // SUB), blank, 0)

    sublane = lax.broadcasted_iota(jnp.int32, (SUB, LANE), 0)
    lane = lax.broadcasted_iota(jnp.int32, (SUB, LANE), 1)
    top, bottom = sublane == 0, sublane == SUB - 1
    first, last = lane == 0, lane == LANE - 1
    nothing = jnp.zeros((SUB, LANE), jnp.float32)

    def columns(tile):
        return pl.ds(tile * LANE, LANE)

    def laplace(field, step, halo, start, use):
        for slot in range(2):
            def row_of(at):
                at = pl.multiple_of(start + at + PAD, SUB)
                return [field[step, slot, pl.ds(at, SUB), columns(t)] for t in range(tiles)]

            above = [pltpu.roll(x, 1, 0) for x in row_of(-SUB)]
            here = row_of(0)
            here_down = [pltpu.roll(x, SUB - 1, 0) for x in here]
            for at in range(0, rows, SUB):
                below = row_of(at + SUB)
                below_down = [pltpu.roll(x, SUB - 1, 0) for x in below]
                here_up = [pltpu.roll(x, 1, 0) for x in here]
                right = [pltpu.roll(x, 1, 1) for x in here]
                left = [pltpu.roll(x, LANE - 1, 1) for x in here]
                row = pl.multiple_of(start + at, SUB)
                for t in range(tiles):
                    value = here[t]
                    beside_y = jnp.where(top, above[t], here_up[t]) + jnp.where(bottom, below_down[t], here_down[t])
                    before = jnp.where(first, right[t - 1] if t else nothing, right[t])
                    after = jnp.where(last, left[t + 1] if t < tiles - 1 else nothing, left[t])
                    other = field[step, 1 - slot, pl.ds(pl.multiple_of(row + PAD, SUB), SUB), columns(t)]
                    across = other + ghost[halo, slot, pl.ds(row, SUB), columns(t)]
                    lap = (across + beside_y + (before + after)) - 6.0 * value
                    use(slot, row, columns(t), value, lap)
                above, here, here_down = here_up, below, below_down

    for load in loads[2:4]:
        load.wait()

    def greet(at):
        for turn in range(len(reach) + 1):
            @pl.when(at == HELLO_TIMES[turn])
            def _():
                if turn > 0:
                    pl.semaphore_wait(hello.at[turn - 1], along_z(reach[turn - 1], lambda device: None))
                if turn < len(reach):
                    along_z(reach[turn], lambda device: pl.semaphore_signal(
                        hello.at[turn], inc=1, device_id=(device,), device_id_type=MESH
                    ))

    def forward(at, carry):
        greet(at)
        step, chunk = at // CHUNKS, lax.rem(at, CHUNKS)
        start = pl.multiple_of(chunk * rows, rows)
        arrived(step, start)

        def use(slot, row, cols, value, lap):
            scaled = time_step * lap
            slopes[step, slot, pl.ds(row, SUB), cols] = scaled
            u[step + 1, slot, pl.ds(pl.multiple_of(row + PAD, SUB), SUB), cols] = (
                value + c[slot, pl.ds(row, SUB), cols] * scaled
            )

        laplace(u, step, step, start, use)
        send(lambda slot: u.at[step + 1, slot, pl.ds(start + PAD, rows), :], step + 1, start)
        return carry

    lax.fori_loop(0, (ITERS - 1) * CHUNKS, forward, 0)
    for load in loads[4:]:
        load.wait()
    totals[0] = nothing

    def turn(chunk, carry):
        start = pl.multiple_of(chunk * rows, rows)
        arrived(ITERS - 1, start)
        sums = [nothing, nothing]

        def use(slot, row, cols, value, lap):
            scaled = time_step * lap
            at = (slot, pl.ds(row, SUB), cols)
            coefficient = c[at]
            resid = value + coefficient * scaled - o[at]
            adjoint = w[at] * resid
            sums[slot] = sums[slot] + adjoint * resid
            lam[at] = adjoint
            grad[at] = adjoint * scaled
            mu[0, slot, pl.ds(pl.multiple_of(row + PAD, SUB), SUB), cols] = coefficient * adjoint

        laplace(u, ITERS - 1, ITERS - 1, start, use)
        send(lambda slot: mu.at[0, slot, pl.ds(start + PAD, rows), :], ITERS, start)
        totals[0] = totals[0] + (sums[0] + sums[1])
        return carry

    lax.fori_loop(0, CHUNKS, turn, 0)

    def pair_copy(stage, device, slot=0):
        return pltpu.make_async_remote_copy(
            src_ref=totals.at[stage],
            dst_ref=inbox.at[stage],
            send_sem=tot_send.at[stage, slot],
            recv_sem=tot_recv.at[stage, slot],
            device_id=(device,),
            device_id_type=MESH,
        )

    def pair_sends(stage, act):
        if stage == 0:
            act(pair_copy(0, beside))
        elif stage < 3:
            upper = lax.rem(column + stage - 1, 2) == 1
            for step, sender in ((1, 0), (-1, 1)):
                @pl.when(jnp.logical_and(core == sender, upper == (step == -1)))
                def _():
                    for c in range(2):
                        act(pair_copy(stage, chip_x(step) + c, c))
        else:
            upper = lax.rem(row + stage - 3, 2) == 1
            act(pair_copy(stage, jnp.where(upper, chip_y(-1), chip_y(1))))

    def pair_there(stage):
        return stage == 0 or (x, x // 2, y, y // 2)[stage - 1] > 1

    def layer_copies():
        return [
            pltpu.make_async_remote_copy(
                src_ref=layers.at[depth],
                dst_ref=layers.at[depth],
                send_sem=layer_send.at[step],
                recv_sem=layer_recv.at[step],
                device_id=(lax.rem(depth + step, z) * layer + lax.rem(me, layer),),
                device_id_type=MESH,
            )
            for step in range(1, z)
        ]

    def exchange(stage):
        if stage < PAIRS:
            if pair_there(stage):
                pair_sends(stage, lambda copy: copy.start())
        else:
            for copy in layer_copies():
                copy.start()

    def collect(stage):
        if stage < PAIRS:
            if not pair_there(stage):
                totals[stage + 1] = totals[stage]
                return
            pair_sends(stage, lambda copy: copy.wait_send())
            if 0 < stage < 3:
                for c in range(2):
                    @pl.when(core == c)
                    def _():
                        pair_copy(stage, beside, c).wait_recv()
            else:
                pair_copy(stage, beside).wait_recv()
            totals[stage + 1] = totals[stage] + inbox[stage]
        else:
            for copy in layer_copies():
                copy.wait()
            total = layers[0]
            for slot in range(1, z):
                total = total + layers[slot]
            totals[stage + 1] = total

    def total_stages(at):
        for stage, (first_at, last_at) in enumerate(STAGE_TIMES):
            @pl.when(at == first_at)
            def _():
                exchange(stage)

            if stage < PAIRS:
                @pl.when(at == last_at)
                def _():
                    collect(stage)
                    if stage == PAIRS - 1:
                        layers[depth] = totals[PAIRS]

    def adjoint(at, carry):
        step, chunk = at // CHUNKS, lax.rem(at, CHUNKS)
        start = pl.multiple_of(chunk * rows, rows)
        total_stages(at)
        arrived(ITERS + step, start)

        def use(slot, row, cols, value, lap):
            at = (slot, pl.ds(row, SUB), cols)
            fresh = lam[at] + time_step * lap
            lam[at] = fresh
            grad[at] = grad[at] + fresh * slopes[ITERS - 2 - step, slot, pl.ds(row, SUB), cols]
            mu[step + 1, slot, pl.ds(pl.multiple_of(row + PAD, SUB), SUB), cols] = c[at] * fresh

        laplace(mu, step, ITERS + step, start, use)
        send(lambda slot: mu.at[step + 1, slot, pl.ds(start + PAD, rows), :], ITERS + step + 1, start)
        return carry

    lax.fori_loop(0, (ITERS - 1) * CHUNKS, adjoint, 0)

    def finish(factor, chunk, carry):
        start = pl.multiple_of(chunk * rows, rows)
        arrived(2 * ITERS - 1, start)

        def use(slot, row, cols, value, lap):
            at = (slot, pl.ds(row, SUB), cols)
            fresh = lam[at] + time_step * lap
            lam[at] = fresh if factor is None else fresh * factor

        laplace(mu, ITERS - 1, 2 * ITERS - 1, start, use)
        return carry

    lax.fori_loop(0, SUM_CHUNK, functools.partial(finish, None), 0)

    collect(PAIRS)
    total = jnp.sum(totals[PAIRS + 1], axis=0, keepdims=True)
    total = jnp.sum(total, axis=1, keepdims=True)
    misfit = jnp.sqrt(jnp.broadcast_to(total, (SUB, LANE)) / (n * 2 * ny * nx) + 1e-06)
    factor = 1.0 / misfit
    misfit_out[...] = misfit

    def divide(field, block, carry):
        row = pl.ds(pl.multiple_of(block * SUB, SUB), SUB)
        for slot in range(2):
            for t in range(tiles):
                at = (slot, row, columns(t))
                field[at] = field[at] * factor
        return carry

    lax.fori_loop(0, ny // SUB, functools.partial(divide, grad), 0)
    lax.fori_loop(0, SUM_CHUNK * rows // SUB, functools.partial(divide, lam), 0)
    lax.fori_loop(SUM_CHUNK, CHUNKS, functools.partial(finish, factor), 0)

    for step in range(2 * ITERS):
        def whole(slot):
            return (u.at[step, slot] if step < ITERS else mu.at[step - ITERS, slot]).at[pl.ds(PAD, ny), :]

        @pl.when(inner)
        def _():
            copy_out(whole(0), step, 0, 0, ny, beyond).wait_send()

        copy_out(whole(1), step, 1, 0, ny, beside).wait_send()


def write_kernel(grad, lam, misfit, grad_out, lam_out, misfit_out, out_sem):
    core = lax.rem(lax.axis_index("gz"), 2)
    copies = [
        pltpu.make_async_copy(source.at[slot], target.at[core if slot == 0 else 1 - core], out_sem.at[which, slot])
        for which, (source, target) in enumerate(((grad, grad_out), (lam, lam_out)))
        for slot in range(2)
    ]
    for copy in copies:
        copy.start()
    misfit_out[0, 0] = misfit[0, 0]
    for copy in copies:
        copy.wait()


def on_device(n, coefficient, initial_field, observed, misfit_weight):
    depth, ny, nx = coefficient.shape
    layers = torus(n)[2]
    far = pl.BlockSpec(memory_space=pltpu.HBM)
    near = pl.BlockSpec(memory_space=pltpu.VMEM)
    slab = jax.ShapeDtypeStruct(coefficient.shape, jnp.float32)
    padded = (ITERS, depth, ny + 2 * PAD, nx)
    gradient, adjoint, misfit = pl.pallas_call(
        functools.partial(kernel, n, ny, nx),
        out_shape=(slab, slab, jax.ShapeDtypeStruct((SUB, LANE), jnp.float32)),
        in_specs=[far] * 4,
        out_specs=(near,) * 3,
        scratch_shapes=[
            pltpu.VMEM(padded, jnp.float32),
            pltpu.VMEM(padded, jnp.float32),
            pltpu.VMEM((ITERS - 1, depth, ny, nx), jnp.float32),
            pltpu.VMEM((depth, ny, nx), jnp.float32),
            pltpu.VMEM((depth, ny, nx), jnp.float32),
            pltpu.VMEM((depth, ny, nx), jnp.float32),
            pltpu.VMEM((2 * ITERS, 2, ny, nx), jnp.float32),
            pltpu.VMEM((PAIRS + 2, SUB, LANE), jnp.float32),
            pltpu.VMEM((PAIRS, SUB, LANE), jnp.float32),
            pltpu.VMEM((layers, SUB, LANE), jnp.float32),
            pltpu.SemaphoreType.DMA((4, 2)),
            pltpu.SemaphoreType.DMA((2 * ITERS, 2)),
            pltpu.SemaphoreType.DMA((2, 2, CHUNKS)),
            pltpu.SemaphoreType.DMA((PAIRS, 2)),
            pltpu.SemaphoreType.DMA((PAIRS, 2)),
            pltpu.SemaphoreType.DMA((layers,)),
            pltpu.SemaphoreType.DMA((layers,)),
            pltpu.SemaphoreType.REGULAR((3,)),
        ],
        compiler_params=pltpu.CompilerParams(
            collective_id=0, has_side_effects=True, vmem_limit_bytes=48 * 1024 * 1024
        ),
    )(coefficient, initial_field, observed, misfit_weight)
    gradient, adjoint, misfit = pl.pallas_call(
        write_kernel,
        out_shape=(slab, slab, jax.ShapeDtypeStruct((1, 1), jnp.float32)),
        in_specs=[near] * 3,
        out_specs=(far, far, pl.BlockSpec(memory_space=pltpu.SMEM)),
        scratch_shapes=[
            pltpu.SemaphoreType.DMA((2, 2)),
        ],
        compiler_params=pltpu.CompilerParams(vmem_limit_bytes=4 * 1024 * 1024),
    )(gradient, adjoint, misfit)
    return gradient, adjoint, misfit.reshape(())


def solution(mesh):
    slab = P("gz", None, None)
    return jax.shard_map(
        functools.partial(on_device, mesh.shape["gz"]),
        mesh=mesh,
        in_specs=(slab,) * 4,
        out_specs=(slab, slab, P()),
        check_vma=False,
    )
```

```python
import functools

import jax
import jax.numpy as jnp
from jax import lax
from jax.experimental import pallas as pl
from jax.experimental.pallas import tpu as pltpu
from jax.sharding import PartitionSpec as P

MESH = pl.DeviceIdType.MESH
time_step = 0.125
ITERS = 4
CHUNKS = 8
PAD = 8
SUB, LANE = 8, 128
SUM_CHUNK = 5
PAIRS = 5
STAGE_TIMES = ((0, 2), (3, 6), (7, 10), (11, 14), (15, 18), (19, None))
HELLO_TIMES = (2, 8, 14, 20)


def torus(n):
    x = min(4, n // 2)
    y = min(4, n // (2 * x))
    return x, y, n // (2 * x * y)


def wait_for(ref, semaphore):
    pltpu.make_async_copy(ref, ref, semaphore).wait()


def kernel(
    n, ny, nx,
    c_hbm, u_hbm, o_hbm, w_hbm,
    grad, lam, misfit_out,
    u, mu, slopes, c, o, w, ghost, totals, inbox, layers,
    load_sem, send_sem, recv_sem, tot_send, tot_recv, layer_sem, hello,
):
    me = lax.axis_index("gz")
    core = lax.rem(me, 2)
    beside = me + 1 - 2 * core
    beyond = me - 1 + 2 * core
    inner = jnp.logical_and(me > 0, me < n - 1)
    x, y, z = torus(n)
    layer = 2 * x * y
    row, column, depth = lax.rem(me // (2 * x), y), lax.rem(me // 2, x), me // layer
    line = me - 2 * column - core

    def chip_x(step):
        return line + 2 * lax.rem(column + step % x, x)

    def chip_y(step):
        return me + 2 * x * (lax.rem(row + step % y, y) - row)

    x_steps = sorted({1 % x, -1 % x} - {0})
    y_steps = sorted({1 % y, -1 % y} - {0})
    partners = [beside] + [chip_x(step) + c for step in x_steps for c in range(2)] + [chip_y(step) for step in y_steps]
    line_end = jnp.logical_and(inner, jnp.where(core == 0, column == 0, column == x - 1))
    reach = [step for step in (1, 2, 4) if step < z]

    def along_z(step, act):
        for away in (step, -step):
            @pl.when(jnp.logical_and(depth + away >= 0, depth + away < z))
            def _():
                act(me + away * layer)

        return (depth >= step).astype(jnp.int32) + (depth + step < z).astype(jnp.int32)

    rows = ny // CHUNKS
    tiles = nx // LANE

    planes = (core, 1 - core)
    loads = []
    for index, (source, target) in enumerate(((u_hbm, u), (c_hbm, c), (o_hbm, o), (w_hbm, w))):
        for slot in range(2):
            place = u.at[0, slot, pl.ds(PAD, ny), :] if target is u else target.at[slot]
            loads.append(pltpu.make_async_copy(source.at[planes[slot]], place, load_sem.at[index]))
    barrier = pltpu.get_barrier_semaphore()

    def ready(device):
        pl.semaphore_signal(barrier, inc=1, device_id=(device,), device_id_type=MESH)

    @pl.when(line_end)
    def _():
        ready(beyond)

    for partner in partners:
        ready(partner)
    others = along_z(1, ready) if reach else 0
    for load in loads[:4]:
        load.start()
    wait_for(u.at[0, :, pl.ds(PAD, ny), :], load_sem.at[0])
    pl.semaphore_wait(barrier, len(partners) + line_end.astype(jnp.int32) + others)

    def copy_out(source, step, slot, start, count, target):
        return pltpu.make_async_remote_copy(
            src_ref=source,
            dst_ref=ghost.at[step, slot, pl.ds(start, count), :],
            send_sem=send_sem.at[slot],
            recv_sem=recv_sem.at[lax.rem(step, 2), start // rows],
            device_id=(target,),
            device_id_type=MESH,
        )

    def send(view, step, start):
        @pl.when(inner)
        def _():
            copy_out(view(0), step, 0, start, rows, beyond).start()

        copy_out(view(1), step, 1, start, rows, beside).start()

    def arrived(step, start):
        @pl.when(inner)
        def _():
            both = ghost.at[step, :, pl.ds(start, rows), :]
            wait_for(both, recv_sem.at[lax.rem(step, 2), start // rows])

        @pl.when(jnp.logical_not(inner))
        def _():
            one = ghost.at[step, 1, pl.ds(start, rows), :]
            wait_for(one, recv_sem.at[lax.rem(step, 2), start // rows])

    for chunk in range(CHUNKS):
        start = chunk * rows
        send(lambda slot: u.at[0, slot, pl.ds(PAD + start, rows), :], 0, start)
    for load in loads[4:]:
        load.start()

    edge = jnp.zeros((SUB, nx), jnp.float32)
    for field, count in ((u, ITERS), (mu, ITERS)):
        for step in range(count):
            for slot in range(2):
                field[step, slot, pl.ds(PAD - SUB, SUB), :] = edge
                field[step, slot, pl.ds(PAD + ny, SUB), :] = edge

    @pl.when(jnp.logical_not(inner))
    def _():
        def blank(at, carry):
            step, row = at // (ny // SUB), lax.rem(at, ny // SUB)
            ghost[step, 0, pl.ds(pl.multiple_of(row * SUB, SUB), SUB), :] = edge
            return carry

        lax.fori_loop(0, 2 * ITERS * (ny // SUB), blank, 0)

    sublane = lax.broadcasted_iota(jnp.int32, (SUB, LANE), 0)
    lane = lax.broadcasted_iota(jnp.int32, (SUB, LANE), 1)
    top, bottom = sublane == 0, sublane == SUB - 1
    first, last = lane == 0, lane == LANE - 1
    nothing = jnp.zeros((SUB, LANE), jnp.float32)

    def columns(tile):
        return pl.ds(tile * LANE, LANE)

    def laplace(field, step, halo, start, use):
        for slot in range(2):
            def row_of(at):
                at = pl.multiple_of(start + at + PAD, SUB)
                return [field[step, slot, pl.ds(at, SUB), columns(t)] for t in range(tiles)]

            above = [pltpu.roll(x, 1, 0) for x in row_of(-SUB)]
            here = row_of(0)
            here_down = [pltpu.roll(x, SUB - 1, 0) for x in here]
            for at in range(0, rows, SUB):
                below = row_of(at + SUB)
                below_down = [pltpu.roll(x, SUB - 1, 0) for x in below]
                here_up = [pltpu.roll(x, 1, 0) for x in here]
                right = [pltpu.roll(x, 1, 1) for x in here]
                left = [pltpu.roll(x, LANE - 1, 1) for x in here]
                row = pl.multiple_of(start + at, SUB)
                for t in range(tiles):
                    value = here[t]
                    beside_y = jnp.where(top, above[t], here_up[t]) + jnp.where(bottom, below_down[t], here_down[t])
                    before = jnp.where(first, right[t - 1] if t else nothing, right[t])
                    after = jnp.where(last, left[t + 1] if t < tiles - 1 else nothing, left[t])
                    other = field[step, 1 - slot, pl.ds(pl.multiple_of(row + PAD, SUB), SUB), columns(t)]
                    across = other + ghost[halo, slot, pl.ds(row, SUB), columns(t)]
                    lap = (across + beside_y + (before + after)) - 6.0 * value
                    use(slot, row, columns(t), value, lap)
                above, here, here_down = here_up, below, below_down

    wait_for(c, load_sem.at[1])

    def greet(at):
        for turn in range(len(reach) + 1):
            @pl.when(at == HELLO_TIMES[turn])
            def _():
                if turn > 0:
                    pl.semaphore_wait(hello.at[turn - 1], along_z(reach[turn - 1], lambda device: None))
                if turn < len(reach):
                    along_z(reach[turn], lambda device: pl.semaphore_signal(
                        hello.at[turn], inc=1, device_id=(device,), device_id_type=MESH
                    ))

    def forward(at, carry):
        greet(at)
        step, chunk = at // CHUNKS, lax.rem(at, CHUNKS)
        start = pl.multiple_of(chunk * rows, rows)
        arrived(step, start)

        def use(slot, row, cols, value, lap):
            scaled = time_step * lap
            slopes[step, slot, pl.ds(row, SUB), cols] = scaled
            u[step + 1, slot, pl.ds(pl.multiple_of(row + PAD, SUB), SUB), cols] = (
                value + c[slot, pl.ds(row, SUB), cols] * scaled
            )

        laplace(u, step, step, start, use)
        send(lambda slot: u.at[step + 1, slot, pl.ds(start + PAD, rows), :], step + 1, start)
        return carry

    lax.fori_loop(0, (ITERS - 1) * CHUNKS, forward, 0)
    wait_for(o, load_sem.at[2])
    wait_for(w, load_sem.at[3])
    totals[0] = nothing

    def turn(chunk, carry):
        start = pl.multiple_of(chunk * rows, rows)
        arrived(ITERS - 1, start)
        sums = [nothing, nothing]

        def use(slot, row, cols, value, lap):
            scaled = time_step * lap
            at = (slot, pl.ds(row, SUB), cols)
            coefficient = c[at]
            resid = value + coefficient * scaled - o[at]
            adjoint = w[at] * resid
            sums[slot] = sums[slot] + adjoint * resid
            lam[at] = adjoint
            grad[at] = adjoint * scaled
            mu[0, slot, pl.ds(pl.multiple_of(row + PAD, SUB), SUB), cols] = coefficient * adjoint

        laplace(u, ITERS - 1, ITERS - 1, start, use)
        send(lambda slot: mu.at[0, slot, pl.ds(start + PAD, rows), :], ITERS, start)
        totals[0] = totals[0] + (sums[0] + sums[1])
        return carry

    lax.fori_loop(0, CHUNKS, turn, 0)

    def pair_copy(stage, device, slot=0):
        return pltpu.make_async_remote_copy(
            src_ref=totals.at[stage],
            dst_ref=inbox.at[stage],
            send_sem=tot_send.at[slot],
            recv_sem=tot_recv.at[stage],
            device_id=(device,),
            device_id_type=MESH,
        )

    def pair_sends(stage, act):
        if stage == 0:
            act(pair_copy(0, beside))
        elif stage < 3:
            upper = lax.rem(column + stage - 1, 2) == 1
            for step, sender in ((1, 0), (-1, 1)):
                @pl.when(jnp.logical_and(core == sender, upper == (step == -1)))
                def _():
                    for c in range(2):
                        act(pair_copy(stage, chip_x(step) + c, c))
        else:
            upper = lax.rem(row + stage - 3, 2) == 1
            act(pair_copy(stage, jnp.where(upper, chip_y(-1), chip_y(1))))

    def pair_there(stage):
        return stage == 0 or (x, x // 2, y, y // 2)[stage - 1] > 1

    def layer_copies():
        return [
            pltpu.make_async_remote_copy(
                src_ref=layers.at[depth],
                dst_ref=layers.at[depth],
                send_sem=layer_sem.at[0],
                recv_sem=layer_sem.at[1],
                device_id=(lax.rem(depth + step, z) * layer + lax.rem(me, layer),),
                device_id_type=MESH,
            )
            for step in range(1, z)
        ]

    def exchange(stage):
        if stage < PAIRS:
            if pair_there(stage):
                pair_sends(stage, lambda copy: copy.start())
        else:
            for copy in layer_copies():
                copy.start()

    def collect(stage):
        if stage < PAIRS:
            if not pair_there(stage):
                totals[stage + 1] = totals[stage]
                return
            pair_sends(stage, lambda copy: copy.wait_send())
            pair_copy(stage, beside).wait_recv()
            totals[stage + 1] = totals[stage] + inbox[stage]
        else:
            if z > 1:
                for index in range(2):
                    wait_for(layers.at[pl.ds(0, z - 1)], layer_sem.at[index])
            total = layers[0]
            for slot in range(1, z):
                total = total + layers[slot]
            totals[stage + 1] = total

    def total_stages(at):
        for stage, (first_at, last_at) in enumerate(STAGE_TIMES):
            @pl.when(at == first_at)
            def _():
                exchange(stage)

            if stage < PAIRS:
                @pl.when(at == last_at)
                def _():
                    collect(stage)
                    if stage == PAIRS - 1:
                        layers[depth] = totals[PAIRS]

    def adjoint(at, carry):
        step, chunk = at // CHUNKS, lax.rem(at, CHUNKS)
        start = pl.multiple_of(chunk * rows, rows)
        total_stages(at)
        arrived(ITERS + step, start)

        def use(slot, row, cols, value, lap):
            at = (slot, pl.ds(row, SUB), cols)
            fresh = lam[at] + time_step * lap
            lam[at] = fresh
            grad[at] = grad[at] + fresh * slopes[ITERS - 2 - step, slot, pl.ds(row, SUB), cols]
            mu[step + 1, slot, pl.ds(pl.multiple_of(row + PAD, SUB), SUB), cols] = c[at] * fresh

        laplace(mu, step, ITERS + step, start, use)
        send(lambda slot: mu.at[step + 1, slot, pl.ds(start + PAD, rows), :], ITERS + step + 1, start)
        return carry

    lax.fori_loop(0, (ITERS - 1) * CHUNKS, adjoint, 0)

    def finish(factor, chunk, carry):
        start = pl.multiple_of(chunk * rows, rows)
        arrived(2 * ITERS - 1, start)

        def use(slot, row, cols, value, lap):
            at = (slot, pl.ds(row, SUB), cols)
            fresh = lam[at] + time_step * lap
            lam[at] = fresh if factor is None else fresh * factor

        laplace(mu, ITERS - 1, 2 * ITERS - 1, start, use)
        return carry

    lax.fori_loop(0, SUM_CHUNK, functools.partial(finish, None), 0)

    collect(PAIRS)
    total = jnp.sum(totals[PAIRS + 1], axis=0, keepdims=True)
    total = jnp.sum(total, axis=1, keepdims=True)
    misfit = jnp.sqrt(jnp.broadcast_to(total, (SUB, LANE)) / (n * 2 * ny * nx) + 1e-06)
    factor = 1.0 / misfit
    misfit_out[...] = misfit

    def divide(field, block, carry):
        row = pl.ds(pl.multiple_of(block * SUB, SUB), SUB)
        for slot in range(2):
            for t in range(tiles):
                at = (slot, row, columns(t))
                field[at] = field[at] * factor
        return carry

    lax.fori_loop(0, ny // SUB, functools.partial(divide, grad), 0)
    lax.fori_loop(0, SUM_CHUNK * rows // SUB, functools.partial(divide, lam), 0)
    lax.fori_loop(SUM_CHUNK, CHUNKS, functools.partial(finish, factor), 0)

    @pl.when(inner)
    def _():
        wait_for(ghost.at[:, 0], send_sem.at[0])

    wait_for(ghost.at[:, 1], send_sem.at[1])


def write_kernel(grad, lam, misfit, grad_out, lam_out, misfit_out, out_sem):
    core = lax.rem(lax.axis_index("gz"), 2)
    copies = [
        pltpu.make_async_copy(source.at[slot], target.at[core if slot == 0 else 1 - core], out_sem.at[which, slot])
        for which, (source, target) in enumerate(((grad, grad_out), (lam, lam_out)))
        for slot in range(2)
    ]
    for copy in copies:
        copy.start()
    misfit_out[0, 0] = misfit[0, 0]
    for copy in copies:
        copy.wait()


def on_device(n, coefficient, initial_field, observed, misfit_weight):
    depth, ny, nx = coefficient.shape
    layers = torus(n)[2]
    far = pl.BlockSpec(memory_space=pltpu.HBM)
    near = pl.BlockSpec(memory_space=pltpu.VMEM)
    slab = jax.ShapeDtypeStruct(coefficient.shape, jnp.float32)
    padded = (ITERS, depth, ny + 2 * PAD, nx)
    gradient, adjoint, misfit = pl.pallas_call(
        functools.partial(kernel, n, ny, nx),
        out_shape=(slab, slab, jax.ShapeDtypeStruct((SUB, LANE), jnp.float32)),
        in_specs=[far] * 4,
        out_specs=(near,) * 3,
        scratch_shapes=[
            pltpu.VMEM(padded, jnp.float32),
            pltpu.VMEM(padded, jnp.float32),
            pltpu.VMEM((ITERS - 1, depth, ny, nx), jnp.float32),
            pltpu.VMEM((depth, ny, nx), jnp.float32),
            pltpu.VMEM((depth, ny, nx), jnp.float32),
            pltpu.VMEM((depth, ny, nx), jnp.float32),
            pltpu.VMEM((2 * ITERS, 2, ny, nx), jnp.float32),
            pltpu.VMEM((PAIRS + 2, SUB, LANE), jnp.float32),
            pltpu.VMEM((PAIRS, SUB, LANE), jnp.float32),
            pltpu.VMEM((layers, SUB, LANE), jnp.float32),
            pltpu.SemaphoreType.DMA((4,)),
            pltpu.SemaphoreType.DMA((2,)),
            pltpu.SemaphoreType.DMA((2, CHUNKS)),
            pltpu.SemaphoreType.DMA((2,)),
            pltpu.SemaphoreType.DMA((PAIRS,)),
            pltpu.SemaphoreType.DMA((2,)),
            pltpu.SemaphoreType.REGULAR((3,)),
        ],
        compiler_params=pltpu.CompilerParams(
            collective_id=0, has_side_effects=True, vmem_limit_bytes=48 * 1024 * 1024
        ),
    )(coefficient, initial_field, observed, misfit_weight)
    gradient, adjoint, misfit = pl.pallas_call(
        write_kernel,
        out_shape=(slab, slab, jax.ShapeDtypeStruct((1, 1), jnp.float32)),
        in_specs=[near] * 3,
        out_specs=(far, far, pl.BlockSpec(memory_space=pltpu.SMEM)),
        scratch_shapes=[
            pltpu.SemaphoreType.DMA((2, 2)),
        ],
        compiler_params=pltpu.CompilerParams(vmem_limit_bytes=4 * 1024 * 1024),
    )(gradient, adjoint, misfit)
    return gradient, adjoint, misfit.reshape(())


def solution(mesh):
    slab = P("gz", None, None)
    return jax.shard_map(
        functools.partial(on_device, mesh.shape["gz"]),
        mesh=mesh,
        in_specs=(slab,) * 4,
        out_specs=(slab, slab, P()),
        check_vma=False,
    )
```

```python
import functools

import jax
import jax.numpy as jnp
from jax import lax
from jax.experimental import pallas as pl
from jax.experimental.pallas import tpu as pltpu
from jax.sharding import PartitionSpec as P

MESH = pl.DeviceIdType.MESH
time_step = 0.125
ITERS = 4
CHUNKS = 8
PAD = 8
SUB, LANE = 8, 128
SUM_CHUNK = 5
PAIRS = 5
STAGE_TIMES = ((0, 2), (3, 6), (7, 10), (11, 14), (15, 18), (19, None))
HELLO_TIMES = (2, 8, 14, 20)


def torus(n):
    x = min(4, n // 2)
    y = min(4, n // (2 * x))
    return x, y, n // (2 * x * y)


def wait_for(ref, semaphore):
    pltpu.make_async_copy(ref, ref, semaphore).wait()


def kernel(
    n, ny, nx,
    c_hbm, u_hbm, o_hbm, w_hbm,
    grad, lam, misfit_out,
    u, mu, slopes, c, o, w, ghost, totals, inbox, layers,
    load_sem, send_sem, recv_sem, tot_send, tot_recv, layer_sem, hello,
):
    me = lax.axis_index("gz")
    core = lax.rem(me, 2)
    beside = me + 1 - 2 * core
    beyond = me - 1 + 2 * core
    inner = jnp.logical_and(me > 0, me < n - 1)
    x, y, z = torus(n)
    layer = 2 * x * y
    row, column, depth = lax.rem(me // (2 * x), y), lax.rem(me // 2, x), me // layer
    line = me - 2 * column - core

    def chip_x(step):
        return line + 2 * lax.rem(column + step % x, x)

    def chip_y(step):
        return me + 2 * x * (lax.rem(row + step % y, y) - row)

    x_steps = sorted({1 % x, -1 % x} - {0})
    y_steps = sorted({1 % y, -1 % y} - {0})
    partners = [beside] + [chip_x(step) + c for step in x_steps for c in range(2)] + [chip_y(step) for step in y_steps]
    line_end = jnp.logical_and(inner, jnp.where(core == 0, column == 0, column == x - 1))
    reach = [step for step in (1, 2, 4) if step < z]

    def along_z(step, act):
        for away in (step, -step):
            @pl.when(jnp.logical_and(depth + away >= 0, depth + away < z))
            def _():
                act(me + away * layer)

        return (depth >= step).astype(jnp.int32) + (depth + step < z).astype(jnp.int32)

    rows = ny // CHUNKS
    tiles = nx // LANE

    planes = (core, 1 - core)
    loads = []
    for index, (source, target) in enumerate(((u_hbm, u), (c_hbm, c), (o_hbm, o), (w_hbm, w))):
        for slot in range(2):
            place = u.at[0, slot, pl.ds(PAD, ny), :] if target is u else target.at[slot]
            loads.append(pltpu.make_async_copy(source.at[planes[slot]], place, load_sem.at[index]))
    barrier = pltpu.get_barrier_semaphore()

    def ready(device):
        pl.semaphore_signal(barrier, inc=1, device_id=(device,), device_id_type=MESH)

    @pl.when(line_end)
    def _():
        ready(beyond)

    for partner in partners:
        ready(partner)
    others = along_z(1, ready) if reach else 0
    for load in loads[:4]:
        load.start()
    wait_for(u.at[0, :, pl.ds(PAD, ny), :], load_sem.at[0])
    pl.semaphore_wait(barrier, len(partners) + line_end.astype(jnp.int32) + others)

    def copy_out(source, step, slot, start, count, target):
        return pltpu.make_async_remote_copy(
            src_ref=source,
            dst_ref=ghost.at[step, slot, pl.ds(start, count), :],
            send_sem=send_sem.at[slot],
            recv_sem=recv_sem.at[lax.rem(step, 2), start // rows],
            device_id=(target,),
            device_id_type=MESH,
        )

    def send(view, step, start):
        @pl.when(inner)
        def _():
            copy_out(view(0), step, 0, start, rows, beyond).start()

        copy_out(view(1), step, 1, start, rows, beside).start()

    def arrived(step, start):
        @pl.when(inner)
        def _():
            both = ghost.at[step, :, pl.ds(start, rows), :]
            wait_for(both, recv_sem.at[lax.rem(step, 2), start // rows])

        @pl.when(jnp.logical_not(inner))
        def _():
            one = ghost.at[step, 1, pl.ds(start, rows), :]
            wait_for(one, recv_sem.at[lax.rem(step, 2), start // rows])

    for chunk in range(CHUNKS):
        start = chunk * rows
        send(lambda slot: u.at[0, slot, pl.ds(PAD + start, rows), :], 0, start)
    for load in loads[4:]:
        load.start()

    edge = jnp.zeros((SUB, nx), jnp.float32)
    for field, count in ((u, ITERS), (mu, ITERS)):
        for step in range(count):
            for slot in range(2):
                field[step, slot, pl.ds(PAD - SUB, SUB), :] = edge
                field[step, slot, pl.ds(PAD + ny, SUB), :] = edge

    @pl.when(jnp.logical_not(inner))
    def _():
        def blank(at, carry):
            step, row = at // (ny // SUB), lax.rem(at, ny // SUB)
            ghost[step, 0, pl.ds(pl.multiple_of(row * SUB, SUB), SUB), :] = edge
            return carry

        lax.fori_loop(0, 2 * ITERS * (ny // SUB), blank, 0)

    sublane = lax.broadcasted_iota(jnp.int32, (SUB, LANE), 0)
    lane = lax.broadcasted_iota(jnp.int32, (SUB, LANE), 1)
    top, bottom = sublane == 0, sublane == SUB - 1
    first, last = lane == 0, lane == LANE - 1
    nothing = jnp.zeros((SUB, LANE), jnp.float32)

    def columns(tile):
        return pl.ds(tile * LANE, LANE)

    def laplace(field, step, halo, start, use):
        for slot in range(2):
            def row_of(at):
                at = pl.multiple_of(start + at + PAD, SUB)
                return [field[step, slot, pl.ds(at, SUB), columns(t)] for t in range(tiles)]

            above = [pltpu.roll(x, 1, 0) for x in row_of(-SUB)]
            here = row_of(0)
            here_down = [pltpu.roll(x, SUB - 1, 0) for x in here]
            for at in range(0, rows, SUB):
                below = row_of(at + SUB)
                below_down = [pltpu.roll(x, SUB - 1, 0) for x in below]
                here_up = [pltpu.roll(x, 1, 0) for x in here]
                right = [pltpu.roll(x, 1, 1) for x in here]
                left = [pltpu.roll(x, LANE - 1, 1) for x in here]
                row = pl.multiple_of(start + at, SUB)
                for t in range(tiles):
                    value = here[t]
                    beside_y = jnp.where(top, above[t], here_up[t]) + jnp.where(bottom, below_down[t], here_down[t])
                    before = jnp.where(first, right[t - 1] if t else nothing, right[t])
                    after = jnp.where(last, left[t + 1] if t < tiles - 1 else nothing, left[t])
                    other = field[step, 1 - slot, pl.ds(pl.multiple_of(row + PAD, SUB), SUB), columns(t)]
                    across = other + ghost[halo, slot, pl.ds(row, SUB), columns(t)]
                    lap = (across + beside_y + (before + after)) - 6.0 * value
                    use(slot, row, columns(t), value, lap)
                above, here, here_down = here_up, below, below_down

    wait_for(c, load_sem.at[1])

    def greet(at):
        for turn in range(len(reach) + 1):
            @pl.when(at == HELLO_TIMES[turn])
            def _():
                if turn > 0:
                    pl.semaphore_wait(hello.at[turn - 1], along_z(reach[turn - 1], lambda device: None))
                if turn < len(reach):
                    along_z(reach[turn], lambda device: pl.semaphore_signal(
                        hello.at[turn], inc=1, device_id=(device,), device_id_type=MESH
                    ))

    def forward(at, carry):
        greet(at)
        step, chunk = at // CHUNKS, lax.rem(at, CHUNKS)
        start = pl.multiple_of(chunk * rows, rows)
        arrived(step, start)

        def use(slot, row, cols, value, lap):
            scaled = time_step * lap
            slopes[step, slot, pl.ds(row, SUB), cols] = scaled
            u[step + 1, slot, pl.ds(pl.multiple_of(row + PAD, SUB), SUB), cols] = (
                value + c[slot, pl.ds(row, SUB), cols] * scaled
            )

        laplace(u, step, step, start, use)
        send(lambda slot: u.at[step + 1, slot, pl.ds(start + PAD, rows), :], step + 1, start)
        return carry

    lax.fori_loop(0, (ITERS - 1) * CHUNKS, forward, 0)
    wait_for(o, load_sem.at[2])
    wait_for(w, load_sem.at[3])
    totals[0] = nothing

    def turn(chunk, carry):
        start = pl.multiple_of(chunk * rows, rows)
        arrived(ITERS - 1, start)
        sums = [nothing, nothing]

        def use(slot, row, cols, value, lap):
            scaled = time_step * lap
            at = (slot, pl.ds(row, SUB), cols)
            coefficient = c[at]
            resid = value + coefficient * scaled - o[at]
            adjoint = w[at] * resid
            sums[slot] = sums[slot] + adjoint * resid
            lam[at] = adjoint
            grad[at] = adjoint * scaled
            mu[0, slot, pl.ds(pl.multiple_of(row + PAD, SUB), SUB), cols] = coefficient * adjoint

        laplace(u, ITERS - 1, ITERS - 1, start, use)
        send(lambda slot: mu.at[0, slot, pl.ds(start + PAD, rows), :], ITERS, start)
        totals[0] = totals[0] + (sums[0] + sums[1])
        return carry

    lax.fori_loop(0, CHUNKS, turn, 0)

    def pair_copy(stage, device, slot=0):
        return pltpu.make_async_remote_copy(
            src_ref=totals.at[stage],
            dst_ref=inbox.at[stage],
            send_sem=tot_send.at[slot],
            recv_sem=tot_recv.at[stage],
            device_id=(device,),
            device_id_type=MESH,
        )

    def pair_sends(stage, act):
        if stage == 0:
            act(pair_copy(0, beside))
        elif stage < 3:
            upper = lax.rem(column + stage - 1, 2) == 1
            for step, sender in ((1, 0), (-1, 1)):
                @pl.when(jnp.logical_and(core == sender, upper == (step == -1)))
                def _():
                    for c in range(2):
                        act(pair_copy(stage, chip_x(step) + c, c))
        else:
            upper = lax.rem(row + stage - 3, 2) == 1
            act(pair_copy(stage, jnp.where(upper, chip_y(-1), chip_y(1))))

    def pair_there(stage):
        return stage == 0 or (x, x // 2, y, y // 2)[stage - 1] > 1

    def layer_copies():
        return [
            pltpu.make_async_remote_copy(
                src_ref=layers.at[depth],
                dst_ref=layers.at[depth],
                send_sem=layer_sem.at[0],
                recv_sem=layer_sem.at[1],
                device_id=(lax.rem(depth + step, z) * layer + lax.rem(me, layer),),
                device_id_type=MESH,
            )
            for step in range(1, z)
        ]

    def exchange(stage):
        if stage < PAIRS:
            if pair_there(stage):
                pair_sends(stage, lambda copy: copy.start())
        else:
            for copy in layer_copies():
                copy.start()

    def collect(stage):
        if stage < PAIRS:
            if not pair_there(stage):
                totals[stage + 1] = totals[stage]
                return
            pair_sends(stage, lambda copy: copy.wait_send())
            pair_copy(stage, beside).wait_recv()
            totals[stage + 1] = totals[stage] + inbox[stage]
        else:
            if z > 1:
                for index in range(2):
                    wait_for(layers.at[pl.ds(0, z - 1)], layer_sem.at[index])
            total = layers[0]
            for slot in range(1, z):
                total = total + layers[slot]
            totals[stage + 1] = total

    def total_stages(at):
        for stage, (first_at, last_at) in enumerate(STAGE_TIMES):
            @pl.when(at == first_at)
            def _():
                exchange(stage)

            if stage < PAIRS:
                @pl.when(at == last_at)
                def _():
                    collect(stage)
                    if stage == PAIRS - 1:
                        layers[depth] = totals[PAIRS]

    def adjoint(at, carry):
        step, chunk = at // CHUNKS, lax.rem(at, CHUNKS)
        start = pl.multiple_of(chunk * rows, rows)
        total_stages(at)
        arrived(ITERS + step, start)

        def use(slot, row, cols, value, lap):
            at = (slot, pl.ds(row, SUB), cols)
            fresh = lam[at] + time_step * lap
            lam[at] = fresh
            grad[at] = grad[at] + fresh * slopes[ITERS - 2 - step, slot, pl.ds(row, SUB), cols]
            mu[step + 1, slot, pl.ds(pl.multiple_of(row + PAD, SUB), SUB), cols] = c[at] * fresh

        laplace(mu, step, ITERS + step, start, use)
        send(lambda slot: mu.at[step + 1, slot, pl.ds(start + PAD, rows), :], ITERS + step + 1, start)
        return carry

    lax.fori_loop(0, (ITERS - 1) * CHUNKS, adjoint, 0)

    def finish(factor, chunk, carry):
        start = pl.multiple_of(chunk * rows, rows)
        arrived(2 * ITERS - 1, start)

        def use(slot, row, cols, value, lap):
            at = (slot, pl.ds(row, SUB), cols)
            fresh = lam[at] + time_step * lap
            lam[at] = fresh if factor is None else fresh * factor

        laplace(mu, ITERS - 1, 2 * ITERS - 1, start, use)
        return carry

    lax.fori_loop(0, SUM_CHUNK, functools.partial(finish, None), 0)

    collect(PAIRS)
    total = jnp.sum(totals[PAIRS + 1], axis=0, keepdims=True)
    total = jnp.sum(total, axis=1, keepdims=True)
    misfit = jnp.sqrt(jnp.broadcast_to(total, (SUB, LANE)) / (n * 2 * ny * nx) + 1e-06)
    factor = 1.0 / misfit
    misfit_out[...] = misfit

    def divide(field, block, carry):
        row = pl.ds(pl.multiple_of(block * SUB, SUB), SUB)
        for slot in range(2):
            for t in range(tiles):
                at = (slot, row, columns(t))
                field[at] = field[at] * factor
        return carry

    lax.fori_loop(0, ny // SUB, functools.partial(divide, grad), 0)
    lax.fori_loop(0, SUM_CHUNK * rows // SUB, functools.partial(divide, lam), 0)
    lax.fori_loop(SUM_CHUNK, CHUNKS, functools.partial(finish, factor), 0)

    @pl.when(inner)
    def _():
        wait_for(ghost.at[:, 0], send_sem.at[0])

    wait_for(ghost.at[:, 1], send_sem.at[1])


def write_kernel(grad, lam, misfit, grad_out, lam_out, misfit_out, scalar, out_sem):
    core = lax.rem(lax.axis_index("gz"), 2)
    copies = [
        pltpu.make_async_copy(source.at[slot], target.at[core if slot == 0 else 1 - core], out_sem.at[which, slot])
        for which, (source, target) in enumerate(((grad, grad_out), (lam, lam_out)))
        for slot in range(2)
    ]
    for copy in copies:
        copy.start()
    scalar[0, 0] = misfit[0, 0]
    copies.append(pltpu.make_async_copy(scalar, misfit_out, out_sem.at[2, 0]))
    copies[-1].start()
    for copy in copies:
        copy.wait()


def on_device(n, coefficient, initial_field, observed, misfit_weight):
    depth, ny, nx = coefficient.shape
    layers = torus(n)[2]
    far = pl.BlockSpec(memory_space=pltpu.HBM)
    near = pl.BlockSpec(memory_space=pltpu.VMEM)
    slab = jax.ShapeDtypeStruct(coefficient.shape, jnp.float32)
    padded = (ITERS, depth, ny + 2 * PAD, nx)
    gradient, adjoint, misfit = pl.pallas_call(
        functools.partial(kernel, n, ny, nx),
        out_shape=(slab, slab, jax.ShapeDtypeStruct((SUB, LANE), jnp.float32)),
        in_specs=[far] * 4,
        out_specs=(near,) * 3,
        scratch_shapes=[
            pltpu.VMEM(padded, jnp.float32),
            pltpu.VMEM(padded, jnp.float32),
            pltpu.VMEM((ITERS - 1, depth, ny, nx), jnp.float32),
            pltpu.VMEM((depth, ny, nx), jnp.float32),
            pltpu.VMEM((depth, ny, nx), jnp.float32),
            pltpu.VMEM((depth, ny, nx), jnp.float32),
            pltpu.VMEM((2 * ITERS, 2, ny, nx), jnp.float32),
            pltpu.VMEM((PAIRS + 2, SUB, LANE), jnp.float32),
            pltpu.VMEM((PAIRS, SUB, LANE), jnp.float32),
            pltpu.VMEM((layers, SUB, LANE), jnp.float32),
            pltpu.SemaphoreType.DMA((4,)),
            pltpu.SemaphoreType.DMA((2,)),
            pltpu.SemaphoreType.DMA((2, CHUNKS)),
            pltpu.SemaphoreType.DMA((2,)),
            pltpu.SemaphoreType.DMA((PAIRS,)),
            pltpu.SemaphoreType.DMA((2,)),
            pltpu.SemaphoreType.REGULAR((3,)),
        ],
        compiler_params=pltpu.CompilerParams(
            collective_id=0, has_side_effects=True, vmem_limit_bytes=48 * 1024 * 1024
        ),
    )(coefficient, initial_field, observed, misfit_weight)
    gradient, adjoint, misfit = pl.pallas_call(
        write_kernel,
        out_shape=(slab, slab, jax.ShapeDtypeStruct((1, 1), jnp.float32)),
        in_specs=[near] * 3,
        out_specs=(far,) * 3,
        scratch_shapes=[
            pltpu.SMEM((1, 1), jnp.float32),
            pltpu.SemaphoreType.DMA((3, 2)),
        ],
        compiler_params=pltpu.CompilerParams(vmem_limit_bytes=4 * 1024 * 1024),
    )(gradient, adjoint, misfit)
    return gradient, adjoint, misfit.reshape(())


def solution(mesh):
    slab = P("gz", None, None)
    return jax.shard_map(
        functools.partial(on_device, mesh.shape["gz"]),
        mesh=mesh,
        in_specs=(slab,) * 4,
        out_specs=(slab, slab, P()),
        check_vma=False,
    )
```

```python
import functools

import jax
import jax.numpy as jnp
from jax import lax
from jax.experimental import pallas as pl
from jax.experimental.pallas import tpu as pltpu
from jax.sharding import PartitionSpec as P

MESH = pl.DeviceIdType.MESH
time_step = 0.125
ITERS = 4
CHUNKS = 16
PAD = 8
SUB, LANE = 8, 128
SUM_CHUNK = 11
PAIRS = 5
STAGE_TIMES = ((0, 4), (5, 12), (13, 20), (21, 28), (29, 36), (37, None))
HELLO_TIMES = (4, 16, 28, 40)


def torus(n):
    x = min(4, n // 2)
    y = min(4, n // (2 * x))
    return x, y, n // (2 * x * y)


def wait_for(ref, semaphore):
    pltpu.make_async_copy(ref, ref, semaphore).wait()


def kernel(
    n, ny, nx,
    c_hbm, u_hbm, o_hbm, w_hbm,
    grad, lam, misfit_out,
    u, mu, slopes, c, o, w, ghost, totals, inbox, layers,
    load_sem, send_sem, recv_sem, tot_send, tot_recv, layer_sem, hello,
):
    me = lax.axis_index("gz")
    core = lax.rem(me, 2)
    beside = me + 1 - 2 * core
    beyond = me - 1 + 2 * core
    inner = jnp.logical_and(me > 0, me < n - 1)
    x, y, z = torus(n)
    layer = 2 * x * y
    row, column, depth = lax.rem(me // (2 * x), y), lax.rem(me // 2, x), me // layer
    line = me - 2 * column - core

    def chip_x(step):
        return line + 2 * lax.rem(column + step % x, x)

    def chip_y(step):
        return me + 2 * x * (lax.rem(row + step % y, y) - row)

    x_steps = sorted({1 % x, -1 % x} - {0})
    y_steps = sorted({1 % y, -1 % y} - {0})
    partners = [beside] + [chip_x(step) + c for step in x_steps for c in range(2)] + [chip_y(step) for step in y_steps]
    line_end = jnp.logical_and(inner, jnp.where(core == 0, column == 0, column == x - 1))
    reach = [step for step in (1, 2, 4) if step < z]

    def along_z(step, act):
        for away in (step, -step):
            @pl.when(jnp.logical_and(depth + away >= 0, depth + away < z))
            def _():
                act(me + away * layer)

        return (depth >= step).astype(jnp.int32) + (depth + step < z).astype(jnp.int32)

    rows = ny // CHUNKS
    tiles = nx // LANE

    planes = (core, 1 - core)
    loads = []
    for index, (source, target) in enumerate(((u_hbm, u), (c_hbm, c), (o_hbm, o), (w_hbm, w))):
        for slot in range(2):
            place = u.at[0, slot, pl.ds(PAD, ny), :] if target is u else target.at[slot]
            loads.append(pltpu.make_async_copy(source.at[planes[slot]], place, load_sem.at[index]))
    barrier = pltpu.get_barrier_semaphore()

    def ready(device):
        pl.semaphore_signal(barrier, inc=1, device_id=(device,), device_id_type=MESH)

    @pl.when(line_end)
    def _():
        ready(beyond)

    for partner in partners:
        ready(partner)
    others = along_z(1, ready) if reach else 0
    for load in loads[:4]:
        load.start()
    wait_for(u.at[0, :, pl.ds(PAD, ny), :], load_sem.at[0])
    pl.semaphore_wait(barrier, len(partners) + line_end.astype(jnp.int32) + others)

    def copy_out(source, step, slot, start, count, target):
        return pltpu.make_async_remote_copy(
            src_ref=source,
            dst_ref=ghost.at[step, slot, pl.ds(start, count), :],
            send_sem=send_sem.at[slot],
            recv_sem=recv_sem.at[lax.rem(step, 2), start // rows],
            device_id=(target,),
            device_id_type=MESH,
        )

    def send(view, step, start):
        @pl.when(inner)
        def _():
            copy_out(view(0), step, 0, start, rows, beyond).start()

        copy_out(view(1), step, 1, start, rows, beside).start()

    def arrived(step, start):
        @pl.when(inner)
        def _():
            both = ghost.at[step, :, pl.ds(start, rows), :]
            wait_for(both, recv_sem.at[lax.rem(step, 2), start // rows])

        @pl.when(jnp.logical_not(inner))
        def _():
            one = ghost.at[step, 1, pl.ds(start, rows), :]
            wait_for(one, recv_sem.at[lax.rem(step, 2), start // rows])

    for chunk in range(CHUNKS):
        start = chunk * rows
        send(lambda slot: u.at[0, slot, pl.ds(PAD + start, rows), :], 0, start)
    for load in loads[4:]:
        load.start()

    edge = jnp.zeros((SUB, nx), jnp.float32)
    for field, count in ((u, ITERS), (mu, ITERS)):
        for step in range(count):
            for slot in range(2):
                field[step, slot, pl.ds(PAD - SUB, SUB), :] = edge
                field[step, slot, pl.ds(PAD + ny, SUB), :] = edge

    @pl.when(jnp.logical_not(inner))
    def _():
        def blank(at, carry):
            step, row = at // (ny // SUB), lax.rem(at, ny // SUB)
            ghost[step, 0, pl.ds(pl.multiple_of(row * SUB, SUB), SUB), :] = edge
            return carry

        lax.fori_loop(0, 2 * ITERS * (ny // SUB), blank, 0)

    sublane = lax.broadcasted_iota(jnp.int32, (SUB, LANE), 0)
    lane = lax.broadcasted_iota(jnp.int32, (SUB, LANE), 1)
    top, bottom = sublane == 0, sublane == SUB - 1
    first, last = lane == 0, lane == LANE - 1
    nothing = jnp.zeros((SUB, LANE), jnp.float32)

    def columns(tile):
        return pl.ds(tile * LANE, LANE)

    def laplace(field, step, halo, start, use):
        for slot in range(2):
            def row_of(at):
                at = pl.multiple_of(start + at + PAD, SUB)
                return [field[step, slot, pl.ds(at, SUB), columns(t)] for t in range(tiles)]

            above = [pltpu.roll(x, 1, 0) for x in row_of(-SUB)]
            here = row_of(0)
            here_down = [pltpu.roll(x, SUB - 1, 0) for x in here]
            for at in range(0, rows, SUB):
                below = row_of(at + SUB)
                below_down = [pltpu.roll(x, SUB - 1, 0) for x in below]
                here_up = [pltpu.roll(x, 1, 0) for x in here]
                right = [pltpu.roll(x, 1, 1) for x in here]
                left = [pltpu.roll(x, LANE - 1, 1) for x in here]
                row = pl.multiple_of(start + at, SUB)
                for t in range(tiles):
                    value = here[t]
                    beside_y = jnp.where(top, above[t], here_up[t]) + jnp.where(bottom, below_down[t], here_down[t])
                    before = jnp.where(first, right[t - 1] if t else nothing, right[t])
                    after = jnp.where(last, left[t + 1] if t < tiles - 1 else nothing, left[t])
                    other = field[step, 1 - slot, pl.ds(pl.multiple_of(row + PAD, SUB), SUB), columns(t)]
                    across = other + ghost[halo, slot, pl.ds(row, SUB), columns(t)]
                    lap = (across + beside_y + (before + after)) - 6.0 * value
                    use(slot, row, columns(t), value, lap)
                above, here, here_down = here_up, below, below_down

    wait_for(c, load_sem.at[1])

    def greet(at):
        for turn in range(len(reach) + 1):
            @pl.when(at == HELLO_TIMES[turn])
            def _():
                if turn > 0:
                    pl.semaphore_wait(hello.at[turn - 1], along_z(reach[turn - 1], lambda device: None))
                if turn < len(reach):
                    along_z(reach[turn], lambda device: pl.semaphore_signal(
                        hello.at[turn], inc=1, device_id=(device,), device_id_type=MESH
                    ))

    def forward(at, carry):
        greet(at)
        step, chunk = at // CHUNKS, lax.rem(at, CHUNKS)
        start = pl.multiple_of(chunk * rows, rows)
        arrived(step, start)

        def use(slot, row, cols, value, lap):
            scaled = time_step * lap
            slopes[step, slot, pl.ds(row, SUB), cols] = scaled
            u[step + 1, slot, pl.ds(pl.multiple_of(row + PAD, SUB), SUB), cols] = (
                value + c[slot, pl.ds(row, SUB), cols] * scaled
            )

        laplace(u, step, step, start, use)
        send(lambda slot: u.at[step + 1, slot, pl.ds(start + PAD, rows), :], step + 1, start)
        return carry

    lax.fori_loop(0, (ITERS - 1) * CHUNKS, forward, 0)
    wait_for(o, load_sem.at[2])
    wait_for(w, load_sem.at[3])
    totals[0] = nothing

    def turn(chunk, carry):
        start = pl.multiple_of(chunk * rows, rows)
        arrived(ITERS - 1, start)
        sums = [nothing, nothing]

        def use(slot, row, cols, value, lap):
            scaled = time_step * lap
            at = (slot, pl.ds(row, SUB), cols)
            coefficient = c[at]
            resid = value + coefficient * scaled - o[at]
            adjoint = w[at] * resid
            sums[slot] = sums[slot] + adjoint * resid
            lam[at] = adjoint
            grad[at] = adjoint * scaled
            mu[0, slot, pl.ds(pl.multiple_of(row + PAD, SUB), SUB), cols] = coefficient * adjoint

        laplace(u, ITERS - 1, ITERS - 1, start, use)
        send(lambda slot: mu.at[0, slot, pl.ds(start + PAD, rows), :], ITERS, start)
        totals[0] = totals[0] + (sums[0] + sums[1])
        return carry

    lax.fori_loop(0, CHUNKS, turn, 0)

    def pair_copy(stage, device, slot=0):
        return pltpu.make_async_remote_copy(
            src_ref=totals.at[stage],
            dst_ref=inbox.at[stage],
            send_sem=tot_send.at[slot],
            recv_sem=tot_recv.at[stage],
            device_id=(device,),
            device_id_type=MESH,
        )

    def pair_sends(stage, act):
        if stage == 0:
            act(pair_copy(0, beside))
        elif stage < 3:
            upper = lax.rem(column + stage - 1, 2) == 1
            for step, sender in ((1, 0), (-1, 1)):
                @pl.when(jnp.logical_and(core == sender, upper == (step == -1)))
                def _():
                    for c in range(2):
                        act(pair_copy(stage, chip_x(step) + c, c))
        else:
            upper = lax.rem(row + stage - 3, 2) == 1
            act(pair_copy(stage, jnp.where(upper, chip_y(-1), chip_y(1))))

    def pair_there(stage):
        return stage == 0 or (x, x // 2, y, y // 2)[stage - 1] > 1

    def layer_copies():
        return [
            pltpu.make_async_remote_copy(
                src_ref=layers.at[depth],
                dst_ref=layers.at[depth],
                send_sem=layer_sem.at[0],
                recv_sem=layer_sem.at[1],
                device_id=(lax.rem(depth + step, z) * layer + lax.rem(me, layer),),
                device_id_type=MESH,
            )
            for step in range(1, z)
        ]

    def exchange(stage):
        if stage < PAIRS:
            if pair_there(stage):
                pair_sends(stage, lambda copy: copy.start())
        else:
            for copy in layer_copies():
                copy.start()

    def collect(stage):
        if stage < PAIRS:
            if not pair_there(stage):
                totals[stage + 1] = totals[stage]
                return
            pair_sends(stage, lambda copy: copy.wait_send())
            pair_copy(stage, beside).wait_recv()
            totals[stage + 1] = totals[stage] + inbox[stage]
        else:
            if z > 1:
                for index in range(2):
                    wait_for(layers.at[pl.ds(0, z - 1)], layer_sem.at[index])
            total = layers[0]
            for slot in range(1, z):
                total = total + layers[slot]
            totals[stage + 1] = total

    def total_stages(at):
        for stage, (first_at, last_at) in enumerate(STAGE_TIMES):
            @pl.when(at == first_at)
            def _():
                exchange(stage)

            if stage < PAIRS:
                @pl.when(at == last_at)
                def _():
                    collect(stage)
                    if stage == PAIRS - 1:
                        layers[depth] = totals[PAIRS]

    def adjoint(at, carry):
        step, chunk = at // CHUNKS, lax.rem(at, CHUNKS)
        start = pl.multiple_of(chunk * rows, rows)
        total_stages(at)
        arrived(ITERS + step, start)

        def use(slot, row, cols, value, lap):
            at = (slot, pl.ds(row, SUB), cols)
            fresh = lam[at] + time_step * lap
            lam[at] = fresh
            grad[at] = grad[at] + fresh * slopes[ITERS - 2 - step, slot, pl.ds(row, SUB), cols]
            mu[step + 1, slot, pl.ds(pl.multiple_of(row + PAD, SUB), SUB), cols] = c[at] * fresh

        laplace(mu, step, ITERS + step, start, use)
        send(lambda slot: mu.at[step + 1, slot, pl.ds(start + PAD, rows), :], ITERS + step + 1, start)
        return carry

    lax.fori_loop(0, (ITERS - 1) * CHUNKS, adjoint, 0)

    def finish(factor, chunk, carry):
        start = pl.multiple_of(chunk * rows, rows)
        arrived(2 * ITERS - 1, start)

        def use(slot, row, cols, value, lap):
            at = (slot, pl.ds(row, SUB), cols)
            fresh = lam[at] + time_step * lap
            lam[at] = fresh if factor is None else fresh * factor

        laplace(mu, ITERS - 1, 2 * ITERS - 1, start, use)
        return carry

    lax.fori_loop(0, SUM_CHUNK, functools.partial(finish, None), 0)

    collect(PAIRS)
    total = jnp.sum(totals[PAIRS + 1], axis=0, keepdims=True)
    total = jnp.sum(total, axis=1, keepdims=True)
    misfit = jnp.sqrt(jnp.broadcast_to(total, (SUB, LANE)) / (n * 2 * ny * nx) + 1e-06)
    factor = 1.0 / misfit
    misfit_out[...] = misfit

    def divide(field, block, carry):
        row = pl.ds(pl.multiple_of(block * SUB, SUB), SUB)
        for slot in range(2):
            for t in range(tiles):
                at = (slot, row, columns(t))
                field[at] = field[at] * factor
        return carry

    lax.fori_loop(0, ny // SUB, functools.partial(divide, grad), 0)
    lax.fori_loop(0, SUM_CHUNK * rows // SUB, functools.partial(divide, lam), 0)
    lax.fori_loop(SUM_CHUNK, CHUNKS, functools.partial(finish, factor), 0)

    @pl.when(inner)
    def _():
        wait_for(ghost.at[:, 0], send_sem.at[0])

    wait_for(ghost.at[:, 1], send_sem.at[1])


def write_kernel(grad, lam, misfit, grad_out, lam_out, misfit_out, scalar, out_sem):
    core = lax.rem(lax.axis_index("gz"), 2)
    copies = [
        pltpu.make_async_copy(source.at[slot], target.at[core if slot == 0 else 1 - core], out_sem.at[which, slot])
        for which, (source, target) in enumerate(((grad, grad_out), (lam, lam_out)))
        for slot in range(2)
    ]
    for copy in copies:
        copy.start()
    scalar[0, 0] = misfit[0, 0]
    copies.append(pltpu.make_async_copy(scalar, misfit_out, out_sem.at[2, 0]))
    copies[-1].start()
    for copy in copies:
        copy.wait()


def on_device(n, coefficient, initial_field, observed, misfit_weight):
    depth, ny, nx = coefficient.shape
    layers = torus(n)[2]
    far = pl.BlockSpec(memory_space=pltpu.HBM)
    near = pl.BlockSpec(memory_space=pltpu.VMEM)
    slab = jax.ShapeDtypeStruct(coefficient.shape, jnp.float32)
    padded = (ITERS, depth, ny + 2 * PAD, nx)
    gradient, adjoint, misfit = pl.pallas_call(
        functools.partial(kernel, n, ny, nx),
        out_shape=(slab, slab, jax.ShapeDtypeStruct((SUB, LANE), jnp.float32)),
        in_specs=[far] * 4,
        out_specs=(near,) * 3,
        scratch_shapes=[
            pltpu.VMEM(padded, jnp.float32),
            pltpu.VMEM(padded, jnp.float32),
            pltpu.VMEM((ITERS - 1, depth, ny, nx), jnp.float32),
            pltpu.VMEM((depth, ny, nx), jnp.float32),
            pltpu.VMEM((depth, ny, nx), jnp.float32),
            pltpu.VMEM((depth, ny, nx), jnp.float32),
            pltpu.VMEM((2 * ITERS, 2, ny, nx), jnp.float32),
            pltpu.VMEM((PAIRS + 2, SUB, LANE), jnp.float32),
            pltpu.VMEM((PAIRS, SUB, LANE), jnp.float32),
            pltpu.VMEM((layers, SUB, LANE), jnp.float32),
            pltpu.SemaphoreType.DMA((4,)),
            pltpu.SemaphoreType.DMA((2,)),
            pltpu.SemaphoreType.DMA((2, CHUNKS)),
            pltpu.SemaphoreType.DMA((2,)),
            pltpu.SemaphoreType.DMA((PAIRS,)),
            pltpu.SemaphoreType.DMA((2,)),
            pltpu.SemaphoreType.REGULAR((3,)),
        ],
        compiler_params=pltpu.CompilerParams(
            collective_id=0, has_side_effects=True, vmem_limit_bytes=48 * 1024 * 1024
        ),
    )(coefficient, initial_field, observed, misfit_weight)
    gradient, adjoint, misfit = pl.pallas_call(
        write_kernel,
        out_shape=(slab, slab, jax.ShapeDtypeStruct((1, 1), jnp.float32)),
        in_specs=[near] * 3,
        out_specs=(far,) * 3,
        scratch_shapes=[
            pltpu.SMEM((1, 1), jnp.float32),
            pltpu.SemaphoreType.DMA((3, 2)),
        ],
        compiler_params=pltpu.CompilerParams(vmem_limit_bytes=4 * 1024 * 1024),
    )(gradient, adjoint, misfit)
    return gradient, adjoint, misfit.reshape(())


def solution(mesh):
    slab = P("gz", None, None)
    return jax.shard_map(
        functools.partial(on_device, mesh.shape["gz"]),
        mesh=mesh,
        in_specs=(slab,) * 4,
        out_specs=(slab, slab, P()),
        check_vma=False,
    )
```
